128 devices in a mesh: grp: 4 (over x), dev: 32 (over z, y, core).
Axes of the slice: x: 4, y: 4, z: 4, core: 2. Of those that a mesh axis runs over, the one named last changes fastest.
Arguments:
- embeddings: bfloat16 [1048576, 256], P(('grp', 'dev'))
- prior_dist: float32 [1048576], P(('grp', 'dev')), may hold values from 1 to 3
- seed_ids: int32 [6, 512], replicated, may hold values from 0 to 1048575, as said below
Outputs:
- min_dist: float32 [1048576], P(('grp', 'dev'))
- group_means: float32 [6, 4], P(None, 'grp')
The draws below stay inside these ranges and needn't reach their ends.
Inputs may be any that keep to these rules, and one draw needn't show every extreme that they name: `seed_ids`: round r's ids all lie in the rows of group r mod 4, that is from (r mod 4) * 262144 to (r mod 4 + 1) * 262144 - 1; ids may repeat.
All inputs are finite; a program needn't handle non-finite values.
Results may differ from the reference program's by a relative error of at most 0.0003.
Values may be sent and summed in bfloat16 or wider, within the bound.
A program may use at most 64 MiB of HBM per device.

```python
import jax
import jax.numpy as jnp
from jax import lax

W = 256
SEEDS = 512
ROUNDS = 6
ROW_DEV = 8192
GROUP_ROWS = 262144
ROWS = 1048576
GROUPS = 4


def draw_embeddings(key, part):
    key_rows, key_scale, key_shift, key_center, key_member = jax.random.split(jax.random.fold_in(key, 11), 5)
    cluster_count = 4 * SEEDS
    member = jax.random.randint(key_member, (ROWS,), 0, cluster_count, dtype=jnp.int32)
    centroids = jax.random.normal(key_center, (cluster_count, W), jnp.float32)
    scales = jnp.exp(jax.random.uniform(key_scale, (cluster_count,), jnp.float32, -0.7, 0.7))
    row_scale = jnp.take(scales, member, axis=0)
    row_center = jnp.take(centroids, member, axis=0)
    noise = jax.random.normal(key_rows, (ROWS, W), jnp.float32)
    values = row_scale[:, None] * (row_center + 0.3 * noise)
    return values.astype(jnp.bfloat16)


def draw_seed_ids(key, part):
    owners = jnp.arange(ROUNDS, dtype=jnp.int32) % GROUPS
    within = jax.random.randint(jax.random.fold_in(key, 23), (ROUNDS, SEEDS), 0, GROUP_ROWS, dtype=jnp.int32)
    return (owners[:, None] * GROUP_ROWS + within).astype(jnp.int32)


def steps_of(own_key, extent, cuts, least, top_value):
    factor_of = 1.0
    for position, blocks in cuts:
        steps = jax.random.uniform(jax.random.fold_in(jax.random.fold_in(own_key, 6), position), (blocks,), jnp.float32, least / len(cuts), top_value / len(cuts))
        factor_of = factor_of * jnp.repeat(jnp.exp(steps), extent[position] // blocks).reshape((-1,) + (1,) * (len(extent) - 1 - position))
    return factor_of


def setup_inputs(seed: int = 0) -> dict:
    key_of = jax.random.split(jax.random.key(seed), 4)
    return {
        "embeddings": draw_embeddings(jax.random.fold_in(key_of[3], 71), 0),
        "prior_dist": jnp.clip(1.0 + 2.0 * jax.random.uniform(key_of[1], (ROWS,), jnp.float32) ** steps_of(key_of[1], (ROWS,), ((0, 128),), -0.2, 0.2), 1.0, 3.0),
        "seed_ids": draw_seed_ids(jax.random.fold_in(key_of[3], 71), 0),
    }


def block_nearest(block, block_norms, centers, seed_norms):
    products = jnp.dot(block, centers.T, preferred_element_type=jnp.float32)
    gaps = jnp.maximum(block_norms[:, None] + seed_norms[None, :] - 2.0 * products, 0.0) / float(W)
    return jnp.min(gaps, axis=1)


def reference(embeddings, prior_dist, seed_ids):
    row_norms = jnp.sum(jnp.square(embeddings.astype(jnp.float32)), axis=1)
    block_count = ROWS // ROW_DEV
    blocks = embeddings.reshape(block_count, ROW_DEV, W)
    norm_blocks = row_norms.reshape(block_count, ROW_DEV)
    current = prior_dist
    means = []
    for round_index in range(ROUNDS):
        centers = jnp.take(embeddings, seed_ids[round_index], axis=0)
        seed_norms = jnp.sum(jnp.square(centers.astype(jnp.float32)), axis=1)

        def one_block(pair):
            return block_nearest(pair[0], pair[1], centers, seed_norms)

        nearest = lax.map(one_block, (blocks, norm_blocks)).reshape(ROWS)
        current = jnp.minimum(current, nearest)
        means.append(jnp.sum(current.reshape(GROUPS, GROUP_ROWS), axis=1) / float(GROUP_ROWS))
    return current, jnp.stack(means)
```

```python
import functools

import jax
import jax.numpy as jnp
from jax import lax
from jax.experimental import pallas as pl
from jax.experimental.pallas import tpu as pltpu
from jax.sharding import PartitionSpec as P

MESH = pl.DeviceIdType.MESH
PICK = 16
CHUNK = 256
LANES = 128


def kernel(
    sizes,
    ids_ref,
    emb_hbm,
    prior_ref,
    dist_ref,
    mean_ref,
    emb,
    wide,
    pick_wide,
    picks,
    parts,
    blocks,
    centers,
    half,
    norms,
    best,
    own_total,
    totals,
    load_sem,
    send_sem,
    part_sem,
    block_sem,
    center_sem,
    total_sem,
):
    groups, devs, rounds, seeds, rows, width = sizes
    me_grp = lax.axis_index("grp")
    me = lax.axis_index("dev")
    base = (me_grp * devs + me) * rows
    share = seeds // devs
    pieces = load_sem.shape[0]
    piece = rows // pieces
    slots = picks.shape[0]

    def load(k):
        return pltpu.make_async_copy(
            emb_hbm.at[pl.ds(k * piece, piece)], emb.at[pl.ds(k * piece, piece)], load_sem.at[k]
        )

    for k in range(pieces):
        load(k).start()

    barrier = pltpu.get_barrier_semaphore()

    @pl.loop(1, devs)
    def _(p):
        pl.semaphore_signal(barrier, inc=1, device_id={"dev": lax.rem(me + p, devs)}, device_id_type=MESH)

    for p in range(1, groups):
        pl.semaphore_signal(
            barrier, inc=1, device_id={"grp": lax.rem(me_grp + p, groups)}, device_id_type=MESH
        )

    wide[pl.ds(rows, 8), :] = jnp.zeros((8, width), jnp.float32)
    for k in range(pieces):
        load(k).wait()

        @pl.loop(0, piece // 128)
        def _(t, k=k):
            at = pl.multiple_of(k * piece + t * 128, 128)
            wide[pl.ds(at, 128), :] = emb[pl.ds(at, 128), :].astype(jnp.float32)

    def pick(slot):
        which = me_grp + groups * slot

        @pl.loop(0, seeds // PICK)
        def _(t):
            for u in range(PICK):
                at = ids_ref[which, t * PICK + u] - base
                inside = (at >= 0) & (at < rows)
                at = jnp.where(inside, at, rows)
                pick_wide[u, :, :] = wide[pl.ds(at, 1), :]
            picks[slot, t, :, :] = pick_wide[...].reshape(PICK, width).astype(jnp.bfloat16)

    def scatter(slot):
        @pl.loop(1, devs)
        def _(p):
            to = lax.rem(me + p, devs)
            pltpu.make_async_remote_copy(
                src_ref=picks.at[slot, to],
                dst_ref=parts.at[slot, me],
                send_sem=send_sem.at[slot],
                recv_sem=part_sem.at[slot],
                device_id={"dev": to},
                device_id_type=MESH,
            ).start()

        parts[slot, pl.ds(me, 1)] = picks[slot, pl.ds(me, 1)]

    def take(slot):
        peers = parts.at[slot, pl.ds(0, devs - 1)]
        pltpu.make_async_copy(peers, peers, part_sem.at[slot]).wait()
        total = jnp.sum(parts[slot].astype(jnp.float32), axis=0)
        blocks[me_grp + groups * slot] = total.astype(jnp.bfloat16)

    def trade(slot):
        index = me_grp + groups * slot
        for p in range(1, groups):
            pltpu.make_async_remote_copy(
                src_ref=blocks.at[index],
                dst_ref=blocks.at[index],
                send_sem=send_sem.at[2 + slot],
                recv_sem=block_sem.at[slot],
                device_id={"grp": lax.rem(me_grp + p, groups)},
                device_id_type=MESH,
            ).start()

    def arrived(ref, sem):
        pltpu.make_async_copy(ref, ref, sem).wait()

    def spread(r):
        @pl.loop(1, devs)
        def _(p):
            pltpu.make_async_remote_copy(
                src_ref=blocks.at[r],
                dst_ref=centers.at[r, me],
                send_sem=send_sem.at[4 + r],
                recv_sem=center_sem.at[r],
                device_id={"dev": lax.rem(me + p, devs)},
                device_id_type=MESH,
            ).start()

        centers[r, pl.ds(me, 1)] = blocks[pl.ds(r, 1)]

    tail = rounds - groups
    pick(0)
    pl.semaphore_wait(barrier, devs - 1 + groups - 1)
    scatter(0)

    @pl.when(me_grp < tail)
    def _():
        pick(1)
        scatter(1)

    ones = jnp.ones((16, width), jnp.bfloat16)

    @pl.loop(0, rows // CHUNK)
    def _(j):
        at = pl.multiple_of(j * CHUNK, CHUNK)
        x = wide[pl.ds(at, CHUNK), :]
        square = x * x
        high = square.astype(jnp.bfloat16)
        low = (square - high.astype(jnp.float32)).astype(jnp.bfloat16)
        over = (((1,), (1,)), ((), ()))
        total = lax.dot_general(ones, high, over, preferred_element_type=jnp.float32)
        total += lax.dot_general(ones, low, over, preferred_element_type=jnp.float32)
        for c in range(CHUNK // LANES):
            norms[pl.ds(j * (CHUNK // LANES) + c, 1), :] = total[0:1, c * LANES : (c + 1) * LANES]

    take(0)
    trade(0)
    arrived(blocks.at[pl.ds(0, groups - 1)], block_sem.at[0])
    for r in range(groups):
        spread(r)

    @pl.when(me_grp < tail)
    def _():
        take(1)
        trade(1)
        arrived(blocks.at[pl.ds(0, tail - 1)], block_sem.at[1])

    @pl.when(me_grp >= tail)
    def _():
        arrived(blocks.at[pl.ds(0, tail)], block_sem.at[1])

    for r in range(groups, rounds):
        spread(r)

    current = prior_ref[...]
    for r in range(rounds):
        arrived(centers.at[r, pl.ds(0, devs - 1)], center_sem.at[r])
        c = centers[r].reshape(seeds, width)
        wide_c = c.astype(jnp.float32)
        half[...] = jnp.broadcast_to(
            0.5 * jnp.sum(wide_c * wide_c, axis=1, keepdims=True), (seeds, LANES)
        )

        @pl.loop(0, rows // CHUNK)
        def _(j, r=r):
            at = pl.multiple_of(j * CHUNK, CHUNK)
            x = emb[pl.ds(at, CHUNK), :]
            c = centers[r].reshape(seeds, width)
            product = lax.dot_general(
                c, x, (((1,), (1,)), ((), ())), preferred_element_type=jnp.float32
            )
            for k in range(CHUNK // LANES):
                short = product[:, k * LANES : (k + 1) * LANES] - half[...]
                best[pl.ds(j * (CHUNK // LANES) + k, 1), :] = jnp.max(short, axis=0, keepdims=True)

        nearest = jnp.maximum(norms[...] - 2.0 * best[...], 0.0) / float(width)
        current = jnp.minimum(current, nearest)
        own_total[pl.ds(r, 1), :] = jnp.sum(current, axis=0, keepdims=True)

    dist_ref[...] = current
    own_total[pl.ds(rounds, 8 - rounds), :] = jnp.zeros((8 - rounds, LANES), jnp.float32)

    @pl.loop(1, devs)
    def _(p):
        pltpu.make_async_remote_copy(
            src_ref=own_total,
            dst_ref=totals.at[me],
            send_sem=send_sem.at[4 + rounds],
            recv_sem=total_sem,
            device_id={"dev": lax.rem(me + p, devs)},
            device_id_type=MESH,
        ).start()

    totals[pl.ds(me, 1)] = own_total[...][None]
    arrived(totals.at[pl.ds(0, devs - 1)], total_sem)
    group_sum = jnp.sum(jnp.sum(totals[...], axis=0), axis=1, keepdims=True)
    mean_ref[...] = jnp.broadcast_to(group_sum / float(rows * devs), (8, LANES))

    arrived(parts.at[0, pl.ds(0, devs - 1)], send_sem.at[0])
    arrived(blocks.at[pl.ds(0, groups - 1)], send_sem.at[2])

    @pl.when(me_grp < tail)
    def _():
        arrived(parts.at[1, pl.ds(0, devs - 1)], send_sem.at[1])
        arrived(blocks.at[pl.ds(0, groups - 1)], send_sem.at[3])

    for r in range(rounds):
        arrived(centers.at[r, pl.ds(0, devs - 1)], send_sem.at[4 + r])
    arrived(totals.at[pl.ds(0, devs - 1)], send_sem.at[4 + rounds])


def body(embeddings, prior_dist, seed_ids):
    rows, width = embeddings.shape
    rounds, seeds = seed_ids.shape
    groups, devs = lax.axis_size("grp"), lax.axis_size("dev")
    share = seeds // devs
    slots = -(-rounds // groups)
    sizes = (groups, devs, rounds, seeds, rows, width)
    vmem = pl.BlockSpec(memory_space=pltpu.VMEM)
    dist, means = pl.pallas_call(
        functools.partial(kernel, sizes),
        name="seeding",
        out_shape=(
            jax.ShapeDtypeStruct((rows // LANES, LANES), jnp.float32),
            jax.ShapeDtypeStruct((8, LANES), jnp.float32),
        ),
        in_specs=[
            pl.BlockSpec(memory_space=pltpu.SMEM),
            pl.BlockSpec(memory_space=pl.ANY),
            vmem,
        ],
        out_specs=(vmem, vmem),
        scratch_shapes=[
            pltpu.VMEM((rows, width), jnp.bfloat16),
            pltpu.VMEM((rows + 8, width), jnp.float32),
            pltpu.VMEM((PICK, 1, width), jnp.float32),
            pltpu.VMEM((slots, devs, share, width), jnp.bfloat16),
            pltpu.VMEM((slots, devs, share, width), jnp.bfloat16),
            pltpu.VMEM((rounds, share, width), jnp.bfloat16),
            pltpu.VMEM((rounds, devs, share, width), jnp.bfloat16),
            pltpu.VMEM((seeds, LANES), jnp.float32),
            pltpu.VMEM((rows // LANES, LANES), jnp.float32),
            pltpu.VMEM((rows // LANES, LANES), jnp.float32),
            pltpu.VMEM((8, LANES), jnp.float32),
            pltpu.VMEM((devs, 8, LANES), jnp.float32),
            pltpu.SemaphoreType.DMA((8,)),
            pltpu.SemaphoreType.DMA((5 + rounds,)),
            pltpu.SemaphoreType.DMA((2,)),
            pltpu.SemaphoreType.DMA((2,)),
            pltpu.SemaphoreType.DMA((rounds,)),
            pltpu.SemaphoreType.DMA,
        ],
        compiler_params=pltpu.CompilerParams(
            collective_id=0, has_side_effects=True, vmem_limit_bytes=56 * 1024 * 1024
        ),
    )(seed_ids, embeddings, prior_dist.reshape(rows // LANES, LANES))
    return dist.reshape(rows), means[:rounds, :1]


def solution(mesh):
    placed = (P(("grp", "dev"), None), P(("grp", "dev")), P())
    return jax.shard_map(
        body,
        mesh=mesh,
        in_specs=placed,
        out_specs=(P(("grp", "dev")), P(None, "grp")),
        check_vma=False,
    )
```

```python
import functools

import jax
import jax.numpy as jnp
from jax import lax
from jax.experimental import pallas as pl
from jax.experimental.pallas import tpu as pltpu
from jax.sharding import PartitionSpec as P

MESH = pl.DeviceIdType.MESH
PICK = 16
CHUNK = 256
LANES = 128
PIECE = 128
PIECES = 7
NORM_ROWS = 16


def tile_of(emb, j):
    return emb[pl.ds(pl.multiple_of(j * CHUNK, CHUNK), CHUNK), :]


def row_norms(emb, norms, accs):
    width = emb.shape[1]
    ones = jnp.ones((NORM_ROWS, width), jnp.bfloat16)
    steps = 4

    @pl.loop(0, emb.shape[0] // CHUNK // (2 * steps))
    def _(t):
        for i in range(steps):
            for q in range(2):
                j = (t * steps + i) * 2 + q
                x = tile_of(emb, j).astype(jnp.float32)
                square = x * x
                high = square.astype(jnp.bfloat16)
                low = (square - high.astype(jnp.float32)).astype(jnp.bfloat16)
                acc = accs[q][PIECES + i]
                for part in (high, low):
                    pltpu.matmul_push_rhs(part, staging_register=0, mxu_index=q, transpose=True)
                    pltpu.matmul_acc_lhs(acc, ones, load_staged_rhs=0)
                total = pltpu.matmul_pop(acc)
                for k in range(CHUNK // LANES):
                    norms[pl.ds(j * (CHUNK // LANES) + k, 1), :] = total[
                        0:1, k * LANES : (k + 1) * LANES
                    ]


def nearest_of(emb, center, half, best, accs):
    devs, share, width = center.shape
    seeds = devs * share
    wide_c = center[...].reshape(seeds, width).astype(jnp.float32)
    half[...] = jnp.broadcast_to(
        0.5 * jnp.sum(wide_c * wide_c, axis=1, keepdims=True), (seeds, LANES)
    )
    trips = emb.shape[0] // CHUNK // 2
    count = 0
    for q in range(2):
        pltpu.matmul_push_rhs(tile_of(emb, q), staging_register=0, mxu_index=q, transpose=True)
    for t in range(trips):
        run = {}
        for p in range(seeds // PIECE):
            lhs = center[pl.ds(p * PIECE // share, PIECE // share)].reshape(PIECE, width)
            use = [accs[q][count % PIECES] for q in range(2)]
            for q in range(2):
                pltpu.matmul_acc_lhs(use[q], lhs, load_staged_rhs=0 if p == 0 else None)
            if p == 0 and t + 1 < trips:
                for q in range(2):
                    pltpu.matmul_push_rhs(
                        tile_of(emb, (t + 1) * 2 + q), staging_register=0, mxu_index=q, transpose=True
                    )
            offset = half[pl.ds(p * PIECE, PIECE), :]
            for q in range(2):
                value = pltpu.matmul_pop(use[q])
                for k in range(CHUNK // LANES):
                    short = value[:, k * LANES : (k + 1) * LANES] - offset
                    short = jnp.max(short.reshape(PIECE // 8, 8, LANES), axis=0)
                    run[q, k] = jnp.maximum(run[q, k], short) if p else short
            count += 1
        for (q, k), value in run.items():
            row = (t * 2 + q) * (CHUNK // LANES) + k
            best[pl.ds(row, 1), :] = jnp.max(value, axis=0, keepdims=True)


def kernel(sizes, *refs):
    specs = [
        pltpu.ACC(q)((rows, CHUNK), jnp.float32)
        for q in range(2)
        for rows in [PIECE] * PIECES + [NORM_ROWS] * 4
    ]

    def inner(*accs):
        half = len(accs) // 2
        run_kernel(sizes, *refs, (accs[:half], accs[half:]))

    pl.run_scoped(inner, *specs)


def run_kernel(
    sizes,
    ids_ref,
    emb_hbm,
    prior_ref,
    dist_ref,
    mean_ref,
    emb,
    wide,
    pick_wide,
    picks,
    parts,
    blocks,
    centers,
    half,
    norms,
    best,
    own_total,
    totals,
    load_sem,
    send_sem,
    part_sem,
    block_sem,
    center_sem,
    total_sem,
    accs,
):
    groups, devs, rounds, seeds, rows, width = sizes
    me_grp = lax.axis_index("grp")
    me = lax.axis_index("dev")
    base = (me_grp * devs + me) * rows
    share = seeds // devs
    pieces = load_sem.shape[0]
    piece = rows // pieces
    slots = picks.shape[0]

    def load(k):
        return pltpu.make_async_copy(
            emb_hbm.at[pl.ds(k * piece, piece)], emb.at[pl.ds(k * piece, piece)], load_sem.at[k]
        )

    for k in range(pieces):
        load(k).start()

    barrier = pltpu.get_barrier_semaphore()

    @pl.loop(1, devs)
    def _(p):
        pl.semaphore_signal(barrier, inc=1, device_id={"dev": lax.rem(me + p, devs)}, device_id_type=MESH)

    for p in range(1, groups):
        pl.semaphore_signal(
            barrier, inc=1, device_id={"grp": lax.rem(me_grp + p, groups)}, device_id_type=MESH
        )

    wide[pl.ds(rows, 8), :] = jnp.zeros((8, width), jnp.float32)
    for k in range(pieces):
        load(k).wait()

        @pl.loop(0, piece // 128)
        def _(t, k=k):
            at = pl.multiple_of(k * piece + t * 128, 128)
            wide[pl.ds(at, 128), :] = emb[pl.ds(at, 128), :].astype(jnp.float32)

    def pick(slot):
        which = me_grp + groups * slot

        @pl.loop(0, seeds // PICK)
        def _(t):
            for u in range(PICK):
                at = ids_ref[which, t * PICK + u] - base
                inside = (at >= 0) & (at < rows)
                at = jnp.where(inside, at, rows)
                pick_wide[u, :, :] = wide[pl.ds(at, 1), :]
            picks[slot, t, :, :] = pick_wide[...].reshape(PICK, width).astype(jnp.bfloat16)

    def scatter(slot):
        @pl.loop(1, devs)
        def _(p):
            to = lax.rem(me + p, devs)
            pltpu.make_async_remote_copy(
                src_ref=picks.at[slot, to],
                dst_ref=parts.at[slot, me],
                send_sem=send_sem.at[slot],
                recv_sem=part_sem.at[slot],
                device_id={"dev": to},
                device_id_type=MESH,
            ).start()

        parts[slot, pl.ds(me, 1)] = picks[slot, pl.ds(me, 1)]

    def take(slot):
        peers = parts.at[slot, pl.ds(0, devs - 1)]
        pltpu.make_async_copy(peers, peers, part_sem.at[slot]).wait()
        total = jnp.sum(parts[slot].astype(jnp.float32), axis=0)
        blocks[me_grp + groups * slot] = total.astype(jnp.bfloat16)

    def trade(slot):
        index = me_grp + groups * slot
        for p in range(1, groups):
            pltpu.make_async_remote_copy(
                src_ref=blocks.at[index],
                dst_ref=blocks.at[index],
                send_sem=send_sem.at[2 + slot],
                recv_sem=block_sem.at[slot],
                device_id={"grp": lax.rem(me_grp + p, groups)},
                device_id_type=MESH,
            ).start()

    def arrived(ref, sem):
        pltpu.make_async_copy(ref, ref, sem).wait()

    def spread(r):
        @pl.loop(1, devs)
        def _(p):
            pltpu.make_async_remote_copy(
                src_ref=blocks.at[r],
                dst_ref=centers.at[r, me],
                send_sem=send_sem.at[4 + r],
                recv_sem=center_sem.at[r],
                device_id={"dev": lax.rem(me + p, devs)},
                device_id_type=MESH,
            ).start()

        centers[r, pl.ds(me, 1)] = blocks[pl.ds(r, 1)]

    tail = rounds - groups
    pick(0)
    pl.semaphore_wait(barrier, devs - 1 + groups - 1)
    scatter(0)

    @pl.when(me_grp < tail)
    def _():
        pick(1)
        scatter(1)

    row_norms(emb, norms, accs)

    take(0)
    trade(0)
    arrived(blocks.at[pl.ds(0, groups - 1)], block_sem.at[0])
    for r in range(groups):
        spread(r)

    @pl.when(me_grp < tail)
    def _():
        take(1)
        trade(1)
        arrived(blocks.at[pl.ds(0, tail - 1)], block_sem.at[1])

    @pl.when(me_grp >= tail)
    def _():
        arrived(blocks.at[pl.ds(0, tail)], block_sem.at[1])

    for r in range(groups, rounds):
        spread(r)

    dist_ref[...] = prior_ref[...]
    own_total[...] = jnp.zeros((8, LANES), jnp.float32)
    @pl.loop(0, rounds)
    def _(r):
        arrived(centers.at[r, pl.ds(0, devs - 1)], center_sem.at[r])
        nearest_of(emb, centers.at[r], half, best, accs)
        nearest = jnp.maximum(norms[...] - 2.0 * best[...], 0.0) / float(width)
        current = jnp.minimum(dist_ref[...], nearest)
        dist_ref[...] = current
        own_total[pl.ds(r, 1), :] = jnp.sum(current, axis=0, keepdims=True)

    @pl.loop(1, devs)
    def _(p):
        pltpu.make_async_remote_copy(
            src_ref=own_total,
            dst_ref=totals.at[me],
            send_sem=send_sem.at[4 + rounds],
            recv_sem=total_sem,
            device_id={"dev": lax.rem(me + p, devs)},
            device_id_type=MESH,
        ).start()

    totals[pl.ds(me, 1)] = own_total[...][None]
    arrived(totals.at[pl.ds(0, devs - 1)], total_sem)
    group_sum = jnp.sum(jnp.sum(totals[...], axis=0), axis=1, keepdims=True)
    mean_ref[...] = jnp.broadcast_to(group_sum / float(rows * devs), (8, LANES))

    arrived(parts.at[0, pl.ds(0, devs - 1)], send_sem.at[0])
    arrived(blocks.at[pl.ds(0, groups - 1)], send_sem.at[2])

    @pl.when(me_grp < tail)
    def _():
        arrived(parts.at[1, pl.ds(0, devs - 1)], send_sem.at[1])
        arrived(blocks.at[pl.ds(0, groups - 1)], send_sem.at[3])

    for r in range(rounds):
        arrived(centers.at[r, pl.ds(0, devs - 1)], send_sem.at[4 + r])
    arrived(totals.at[pl.ds(0, devs - 1)], send_sem.at[4 + rounds])


def body(embeddings, prior_dist, seed_ids):
    rows, width = embeddings.shape
    rounds, seeds = seed_ids.shape
    groups, devs = lax.axis_size("grp"), lax.axis_size("dev")
    share = seeds // devs
    slots = -(-rounds // groups)
    sizes = (groups, devs, rounds, seeds, rows, width)
    vmem = pl.BlockSpec(memory_space=pltpu.VMEM)
    dist, means = pl.pallas_call(
        functools.partial(kernel, sizes),
        name="seeding",
        out_shape=(
            jax.ShapeDtypeStruct((rows // LANES, LANES), jnp.float32),
            jax.ShapeDtypeStruct((8, LANES), jnp.float32),
        ),
        in_specs=[
            pl.BlockSpec(memory_space=pltpu.SMEM),
            pl.BlockSpec(memory_space=pl.ANY),
            vmem,
        ],
        out_specs=(vmem, vmem),
        scratch_shapes=[
            pltpu.VMEM((rows, width), jnp.bfloat16),
            pltpu.VMEM((rows + 8, width), jnp.float32),
            pltpu.VMEM((PICK, 1, width), jnp.float32),
            pltpu.VMEM((slots, devs, share, width), jnp.bfloat16),
            pltpu.VMEM((slots, devs, share, width), jnp.bfloat16),
            pltpu.VMEM((rounds, share, width), jnp.bfloat16),
            pltpu.VMEM((rounds, devs, share, width), jnp.bfloat16),
            pltpu.VMEM((seeds, LANES), jnp.float32),
            pltpu.VMEM((rows // LANES, LANES), jnp.float32),
            pltpu.VMEM((rows // LANES, LANES), jnp.float32),
            pltpu.VMEM((8, LANES), jnp.float32),
            pltpu.VMEM((devs, 8, LANES), jnp.float32),
            pltpu.SemaphoreType.DMA((8,)),
            pltpu.SemaphoreType.DMA((5 + rounds,)),
            pltpu.SemaphoreType.DMA((2,)),
            pltpu.SemaphoreType.DMA((2,)),
            pltpu.SemaphoreType.DMA((rounds,)),
            pltpu.SemaphoreType.DMA,
        ],
        compiler_params=pltpu.CompilerParams(
            collective_id=0, has_side_effects=True, vmem_limit_bytes=56 * 1024 * 1024
        ),
    )(seed_ids, embeddings, prior_dist.reshape(rows // LANES, LANES))
    return dist.reshape(rows), means[:rounds, :1]


def solution(mesh):
    placed = (P(("grp", "dev"), None), P(("grp", "dev")), P())
    return jax.shard_map(
        body,
        mesh=mesh,
        in_specs=placed,
        out_specs=(P(("grp", "dev")), P(None, "grp")),
        check_vma=False,
    )
```

```python
import functools

import jax
import jax.numpy as jnp
from jax import lax
from jax.experimental import pallas as pl
from jax.experimental.pallas import tpu as pltpu
from jax.sharding import PartitionSpec as P

MESH = pl.DeviceIdType.MESH
PICK = 32
CHUNK = 256
LANES = 128
PIECE = 128
PIECES = 7
NORM_ROWS = 16


def tile_of(emb, j):
    return emb[pl.ds(pl.multiple_of(j * CHUNK, CHUNK), CHUNK), :]


def row_norms(emb, norms, accs):
    width = emb.shape[1]
    ones = jnp.ones((NORM_ROWS, width), jnp.bfloat16)
    steps = 4

    @pl.loop(0, emb.shape[0] // CHUNK // (2 * steps))
    def _(t):
        for i in range(steps):
            for q in range(2):
                j = (t * steps + i) * 2 + q
                x = tile_of(emb, j).astype(jnp.float32)
                square = x * x
                high = square.astype(jnp.bfloat16)
                low = (square - high.astype(jnp.float32)).astype(jnp.bfloat16)
                acc = accs[q][PIECES + i]
                for part in (high, low):
                    pltpu.matmul_push_rhs(part, staging_register=0, mxu_index=q, transpose=True)
                    pltpu.matmul_acc_lhs(acc, ones, load_staged_rhs=0)
                total = pltpu.matmul_pop(acc)
                for k in range(CHUNK // LANES):
                    norms[pl.ds(j * (CHUNK // LANES) + k, 1), :] = total[
                        0:1, k * LANES : (k + 1) * LANES
                    ]


def nearest_of(emb, center, half, best, accs, middle):
    cores, chips, share, width = center.shape
    seeds = cores * chips * share
    side = chips * share
    wide_c = center[...].reshape(seeds, width).astype(jnp.float32)
    half[...] = jnp.broadcast_to(
        0.5 * jnp.sum(wide_c * wide_c, axis=1, keepdims=True), (seeds, LANES)
    )
    trips = emb.shape[0] // CHUNK // 2
    count = 0
    for q in range(2):
        pltpu.matmul_push_rhs(tile_of(emb, q), staging_register=0, mxu_index=q, transpose=True)
    for t in range(trips):
        if t == trips // 2:
            middle()
        run = {}
        for p in range(seeds // PIECE):
            at = p * PIECE % side // share
            lhs = center[p * PIECE // side, pl.ds(at, PIECE // share)].reshape(PIECE, width)
            use = [accs[q][count % PIECES] for q in range(2)]
            for q in range(2):
                pltpu.matmul_acc_lhs(use[q], lhs, load_staged_rhs=0 if p == 0 else None)
            if p == 0 and t + 1 < trips:
                for q in range(2):
                    pltpu.matmul_push_rhs(
                        tile_of(emb, (t + 1) * 2 + q), staging_register=0, mxu_index=q, transpose=True
                    )
            offset = half[pl.ds(p * PIECE, PIECE), :]
            for q in range(2):
                value = pltpu.matmul_pop(use[q])
                for k in range(CHUNK // LANES):
                    short = value[:, k * LANES : (k + 1) * LANES] - offset
                    short = jnp.max(short.reshape(PIECE // 8, 8, LANES), axis=0)
                    run[q, k] = jnp.maximum(run[q, k], short) if p else short
            count += 1
        for (q, k), value in run.items():
            row = (t * 2 + q) * (CHUNK // LANES) + k
            best[pl.ds(row, 1), :] = jnp.max(value, axis=0, keepdims=True)


def kernel(sizes, *refs):
    specs = [
        pltpu.ACC(q)((rows, CHUNK), jnp.float32)
        for q in range(2)
        for rows in [PIECE] * PIECES + [NORM_ROWS] * 4
    ]

    def inner(*accs):
        half = len(accs) // 2
        run_kernel(sizes, *refs, (accs[:half], accs[half:]))

    pl.run_scoped(inner, *specs)


def arrived(ref, sem):
    pltpu.make_async_copy(ref, ref, sem).wait()


def run_kernel(
    sizes,
    ids_hbm,
    emb_hbm,
    prior_hbm,
    dist_ref,
    mean_ref,
    ids,
    emb,
    prior,
    wide,
    pick_wide,
    picks,
    parts,
    blocks,
    centers,
    half,
    norms,
    best,
    nearest,
    own_rows,
    own_total,
    totals,
    load_sem,
    id_sem,
    prior_sem,
    send_sem,
    part_sem,
    block_sem,
    center_sem,
    relay_sem,
    total_sem,
    accs,
):
    groups, devs, rounds, seeds, rows, width = sizes
    me_grp = lax.axis_index("grp")
    me = lax.axis_index("dev")
    cores = 2
    chips = devs // cores
    chip, core = me // cores, lax.rem(me, cores)
    base = (me_grp * devs + me) * rows
    share = seeds // devs
    pieces = load_sem.shape[0]
    piece = rows // pieces
    tail = rounds - groups

    def load(k):
        return pltpu.make_async_copy(
            emb_hbm.at[pl.ds(k * piece, piece)], emb.at[pl.ds(k * piece, piece)], load_sem.at[k]
        )

    def load_ids(slot):
        which = me_grp + groups * slot
        return pltpu.make_async_copy(
            ids_hbm.at[pl.ds(which, 1)], ids.at[pl.ds(slot, 1)], id_sem.at[slot]
        )

    load_ids(0).start()
    for k in range(pieces):
        load(k).start()
    load_prior = pltpu.make_async_copy(prior_hbm, prior, prior_sem)
    load_prior.start()

    @pl.when(me_grp < tail)
    def _():
        load_ids(1).start()

    barrier = pltpu.get_barrier_semaphore()

    @pl.loop(1, devs)
    def _(p):
        pl.semaphore_signal(barrier, inc=1, device_id={"dev": lax.rem(me + p, devs)}, device_id_type=MESH)

    for p in range(1, groups):
        pl.semaphore_signal(
            barrier, inc=1, device_id={"grp": lax.rem(me_grp + p, groups)}, device_id_type=MESH
        )

    wide[pl.ds(2 * rows, 16), :] = jnp.zeros((16, LANES), jnp.float32)
    for k in range(pieces):
        load(k).wait()

        @pl.loop(0, piece // 128)
        def _(t, k=k):
            at = pl.multiple_of(k * piece + t * 128, 128)
            x = emb[pl.ds(at, 128), :].astype(jnp.float32)
            for h in range(2):
                wide[pl.ds(2 * at + h, 128, stride=2), :] = x[:, h * LANES : (h + 1) * LANES]

    def pick(slot):
        load_ids(slot).wait()

        @pl.loop(0, seeds // PICK)
        def _(t):
            for u in range(PICK):
                at = ids[slot, t * PICK + u] - base
                inside = (at >= 0) & (at < rows)
                at = jnp.where(inside, 2 * at, 2 * rows)
                pick_wide[pl.ds(2 * (t * PICK + u), 2), :] = wide[pl.ds(at, 2), :]

        @pl.loop(0, devs, unroll=4)
        def _(t):
            for h in range(2):
                picks[slot, t, :, h * LANES : (h + 1) * LANES] = pick_wide[
                    pl.ds(2 * share * t + h, share, stride=2), :
                ].astype(jnp.bfloat16)

    def scatter(slot):
        @pl.loop(1, devs)
        def _(p):
            to = lax.rem(me + p, devs)
            pltpu.make_async_remote_copy(
                src_ref=picks.at[slot, to],
                dst_ref=parts.at[slot, me],
                send_sem=send_sem.at[slot],
                recv_sem=part_sem.at[slot],
                device_id={"dev": to},
                device_id_type=MESH,
            ).start()

        parts[slot, pl.ds(me, 1)] = picks[slot, pl.ds(me, 1)]

    def take(slot):
        arrived(parts.at[slot, pl.ds(0, devs - 1)], part_sem.at[slot])
        total = jnp.sum(parts[slot].astype(jnp.float32), axis=0)
        blocks[me_grp + groups * slot] = total.astype(jnp.bfloat16)

    def trade(slot):
        index = me_grp + groups * slot
        for p in range(1, groups):
            pltpu.make_async_remote_copy(
                src_ref=blocks.at[index],
                dst_ref=blocks.at[index],
                send_sem=send_sem.at[2 + slot],
                recv_sem=block_sem.at[slot],
                device_id={"grp": lax.rem(me_grp + p, groups)},
                device_id_type=MESH,
            ).start()

    def spread(r):
        @pl.loop(1, chips)
        def _(p):
            pltpu.make_async_remote_copy(
                src_ref=blocks.at[r],
                dst_ref=centers.at[r, core, chip],
                send_sem=send_sem.at[4 + r],
                recv_sem=center_sem.at[r],
                device_id={"dev": lax.rem(chip + p, chips) * cores + core},
                device_id_type=MESH,
            ).start()

        centers[r, core, chip] = blocks[r]

    def relay(r):
        arrived(centers.at[r, 0, pl.ds(0, chips - 1)], center_sem.at[r])
        pltpu.make_async_remote_copy(
            src_ref=centers.at[r, core],
            dst_ref=centers.at[r, core],
            send_sem=send_sem.at[4 + rounds + r],
            recv_sem=relay_sem.at[r],
            device_id={"dev": chip * cores + 1 - core},
            device_id_type=MESH,
        ).start()

    def turn(i):
        lap = i // groups
        return lap * groups + lax.rem(me_grp * (1 - lap) + i, groups)

    pick(0)
    pl.semaphore_wait(barrier, devs - 1 + groups - 1)
    scatter(0)
    row_norms(emb, norms, accs)

    @pl.when(me_grp < tail)
    def _():
        pick(1)

    take(0)
    spread(me_grp)
    trade(0)

    @pl.when(me_grp < tail)
    def _():
        scatter(1)

    arrived(blocks.at[pl.ds(0, groups - 1)], block_sem.at[0])
    for i in range(1, groups):
        spread(turn(i))
    relay(me_grp)

    @pl.loop(0, rounds)
    def _(i):
        r = turn(i)
        arrived(centers.at[r, 0], relay_sem.at[r])

        def middle():
            @pl.when(i + 1 < rounds)
            def _():
                relay(turn(i + 1))

            @pl.when((i == 0) & (me_grp < tail))
            def _():
                take(1)
                trade(1)

            @pl.when(i == 1)
            def _():
                @pl.when(me_grp < tail)
                def _():
                    arrived(blocks.at[pl.ds(0, tail - 1)], block_sem.at[1])

                @pl.when(me_grp >= tail)
                def _():
                    arrived(blocks.at[pl.ds(0, tail)], block_sem.at[1])

                for s in range(groups, rounds):
                    spread(s)

        nearest_of(emb, centers.at[r], half, best, accs, middle)
        nearest[r] = jnp.maximum(norms[...] - 2.0 * best[...], 0.0) / float(width)

    load_prior.wait()
    current = prior[...]
    own_rows[...] = jnp.zeros((8, LANES), jnp.float32)
    for r in range(rounds):
        current = jnp.minimum(current, nearest[r])
        own_rows[pl.ds(r, 1), :] = jnp.sum(current, axis=0, keepdims=True)
    dist_ref[...] = current
    sums = jnp.broadcast_to(jnp.sum(own_rows[...], axis=1, keepdims=True), (8, LANES))
    lane = lax.broadcasted_iota(jnp.int32, (8, LANES), 1)
    row = lax.broadcasted_iota(jnp.int32, (8, LANES), 0)
    own_total[...] = jnp.sum(jnp.where(lane == row, sums, 0.0), axis=0, keepdims=True)

    @pl.loop(1, devs)
    def _(p):
        pltpu.make_async_remote_copy(
            src_ref=own_total,
            dst_ref=totals.at[me],
            send_sem=send_sem.at[4 + 2 * rounds],
            recv_sem=total_sem,
            device_id={"dev": lax.rem(me + p, devs)},
            device_id_type=MESH,
        ).start()

    totals[pl.ds(me, 1)] = own_total[...][None]
    arrived(totals.at[pl.ds(0, devs - 1)], total_sem)
    mean_ref[...] = jnp.sum(totals[...], axis=0) / float(rows * devs)

    arrived(parts.at[0, pl.ds(0, devs - 1)], send_sem.at[0])
    arrived(blocks.at[pl.ds(0, groups - 1)], send_sem.at[2])

    @pl.when(me_grp < tail)
    def _():
        arrived(parts.at[1, pl.ds(0, devs - 1)], send_sem.at[1])
        arrived(blocks.at[pl.ds(0, groups - 1)], send_sem.at[3])

    for r in range(rounds):
        arrived(centers.at[r, 0, pl.ds(0, chips - 1)], send_sem.at[4 + r])
        arrived(centers.at[r, 0], send_sem.at[4 + rounds + r])
    arrived(totals.at[pl.ds(0, devs - 1)], send_sem.at[4 + 2 * rounds])


def finish(dist_in, mean_in, dist_ref, mean_ref):
    dist_ref[...] = dist_in[...]
    mean_ref[...] = mean_in[:, : mean_ref.shape[1]]


def body(embeddings, prior_dist, seed_ids):
    rows, width = embeddings.shape
    rounds, seeds = seed_ids.shape
    groups, devs = lax.axis_size("grp"), lax.axis_size("dev")
    share = seeds // devs
    slots = -(-rounds // groups)
    sizes = (groups, devs, rounds, seeds, rows, width)
    flat = (rows // LANES, LANES)
    vmem = pl.BlockSpec(memory_space=pltpu.VMEM)
    hbm = pl.BlockSpec(memory_space=pltpu.HBM)
    dist, means = pl.pallas_call(
        functools.partial(kernel, sizes),
        name="seeding",
        out_shape=(
            jax.ShapeDtypeStruct(flat, jnp.float32),
            jax.ShapeDtypeStruct((1, LANES), jnp.float32),
        ),
        in_specs=[hbm, hbm, hbm],
        out_specs=(vmem, vmem),
        scratch_shapes=[
            pltpu.SMEM((slots, seeds), jnp.int32),
            pltpu.VMEM((rows, width), jnp.bfloat16),
            pltpu.VMEM(flat, jnp.float32),
            pltpu.VMEM((2 * rows + 16, LANES), jnp.float32),
            pltpu.VMEM((2 * seeds, LANES), jnp.float32),
            pltpu.VMEM((slots, devs, share, width), jnp.bfloat16),
            pltpu.VMEM((slots, devs, share, width), jnp.bfloat16),
            pltpu.VMEM((rounds, share, width), jnp.bfloat16),
            pltpu.VMEM((rounds, 2, devs // 2, share, width), jnp.bfloat16),
            pltpu.VMEM((seeds, LANES), jnp.float32),
            pltpu.VMEM(flat, jnp.float32),
            pltpu.VMEM(flat, jnp.float32),
            pltpu.VMEM((rounds, *flat), jnp.float32),
            pltpu.VMEM((8, LANES), jnp.float32),
            pltpu.VMEM((1, LANES), jnp.float32),
            pltpu.VMEM((devs, 1, LANES), jnp.float32),
            pltpu.SemaphoreType.DMA((8,)),
            pltpu.SemaphoreType.DMA((slots,)),
            pltpu.SemaphoreType.DMA,
            pltpu.SemaphoreType.DMA((5 + 2 * rounds,)),
            pltpu.SemaphoreType.DMA((2,)),
            pltpu.SemaphoreType.DMA((2,)),
            pltpu.SemaphoreType.DMA((rounds,)),
            pltpu.SemaphoreType.DMA((rounds,)),
            pltpu.SemaphoreType.DMA,
        ],
        compiler_params=pltpu.CompilerParams(
            collective_id=0, has_side_effects=True, vmem_limit_bytes=67_000_000
        ),
    )(seed_ids, embeddings, prior_dist.reshape(flat))
    dist, means = pl.pallas_call(
        finish,
        name="finish",
        out_shape=(
            jax.ShapeDtypeStruct(flat, jnp.float32),
            jax.ShapeDtypeStruct((1, rounds), jnp.float32),
        ),
        in_specs=[vmem, vmem],
        out_specs=(vmem, vmem),
        compiler_params=pltpu.CompilerParams(vmem_limit_bytes=1024 * 1024),
    )(dist, means)
    return dist.reshape(rows), means.reshape(rounds, 1)


def solution(mesh):
    placed = (P(("grp", "dev"), None), P(("grp", "dev")), P())
    return jax.shard_map(
        body,
        mesh=mesh,
        in_specs=placed,
        out_specs=(P(("grp", "dev")), P(None, "grp")),
        check_vma=False,
    )
```

```python
import functools

import jax
import jax.numpy as jnp
from jax import lax
from jax.experimental import pallas as pl
from jax.experimental.pallas import tpu as pltpu
from jax.sharding import PartitionSpec as P

MESH = pl.DeviceIdType.MESH
PICK = 32
CHUNK = 256
LANES = 128
PIECE = 128
PIECES = 7
LAG = 4
EDGE = 8
NORM_ROWS = 16


def tile_of(emb, j):
    return emb[pl.ds(pl.multiple_of(j * CHUNK, CHUNK), CHUNK), :]


def row_norms(emb, norms, accs):
    width = emb.shape[1]
    ones = jnp.ones((NORM_ROWS, width), jnp.bfloat16)
    steps = 4

    @pl.loop(0, emb.shape[0] // CHUNK // (2 * steps))
    def _(t):
        for i in range(steps):
            for q in range(2):
                j = (t * steps + i) * 2 + q
                x = tile_of(emb, j).astype(jnp.float32)
                square = x * x
                high = square.astype(jnp.bfloat16)
                low = (square - high.astype(jnp.float32)).astype(jnp.bfloat16)
                acc = accs[q][PIECES + i]
                for part in (high, low):
                    pltpu.matmul_push_rhs(part, staging_register=0, mxu_index=q, transpose=True)
                    pltpu.matmul_acc_lhs(acc, ones, load_staged_rhs=0)
                total = pltpu.matmul_pop(acc)
                for k in range(CHUNK // LANES):
                    norms[pl.ds(j * (CHUNK // LANES) + k, 1), :] = total[
                        0:1, k * LANES : (k + 1) * LANES
                    ]


def push_tiles(emb, t):
    for q in range(2):
        pltpu.matmul_push_rhs(
            tile_of(emb, t * 2 + q), staging_register=0, mxu_index=q, transpose=True
        )


def half_norms(center, half, unit):
    chips, share, width = center.shape
    wide_c = center[...].reshape(chips * share, width).astype(jnp.float32)
    half[unit] = jnp.broadcast_to(
        0.5 * jnp.sum(wide_c * wide_c, axis=1, keepdims=True), (chips * share, LANES)
    )


def nearest_of(emb, sides, half, best, accs, between):
    chips, share, width = sides[0].shape
    trips = emb.shape[0] // CHUNK // 2
    pieces = chips * share // PIECE
    pending = []
    run = {}

    def pop():
        unit, t, p, use = pending.pop(0)
        offset = half[unit, pl.ds(p * PIECE, PIECE), :]
        for q in range(2):
            value = pltpu.matmul_pop(use[q])
            for k in range(CHUNK // LANES):
                short = value[:, k * LANES : (k + 1) * LANES] - offset
                short = jnp.max(short.reshape(PIECE // 8, 8, LANES), axis=0)
                run[q, k] = jnp.maximum(run[q, k], short) if p else short
        if p == pieces - 1:
            for (q, k), value in list(run.items()):
                row = (t * 2 + q) * (CHUNK // LANES) + k
                value = jnp.max(value, axis=0, keepdims=True)
                if unit:
                    value = jnp.maximum(value, best[pl.ds(row, 1), :])
                best[pl.ds(row, 1), :] = value

    count = 0
    for unit in range(2):
        if unit:
            between()
        half_norms(sides[unit], half, unit)
        for t in range(trips):
            for p in range(pieces):
                lhs = sides[unit][pl.ds(p * PIECE // share, PIECE // share)].reshape(PIECE, width)
                use = [accs[q][count % PIECES] for q in range(2)]
                count += 1
                for q in range(2):
                    pltpu.matmul_acc_lhs(use[q], lhs, load_staged_rhs=None if p else 0)
                if p == 0:
                    push_tiles(emb, (t + 1) % trips)
                pending.append((unit, t, p, use))
                if len(pending) > LAG:
                    pop()
    while pending:
        pop()


def kernel(sizes, *refs):
    specs = [
        pltpu.ACC(q)((rows, CHUNK), jnp.float32)
        for q in range(2)
        for rows in [PIECE] * PIECES + [NORM_ROWS] * 4
    ]

    def inner(*accs):
        half = len(accs) // 2
        run_kernel(sizes, *refs, (accs[:half], accs[half:]))

    pl.run_scoped(inner, *specs)


def arrived(ref, sem):
    pltpu.make_async_copy(ref, ref, sem).wait()


def run_kernel(
    sizes,
    ids_hbm,
    emb_hbm,
    prior_hbm,
    both_ref,
    ids,
    emb,
    prior,
    wide,
    pick_wide,
    picks,
    parts,
    blocks,
    centers,
    half,
    norms,
    best,
    nearest,
    own_rows,
    own_total,
    totals,
    load_sem,
    id_sem,
    prior_sem,
    send_sem,
    part_sem,
    block_sem,
    center_sem,
    relay_sem,
    total_sem,
    accs,
):
    groups, devs, rounds, seeds, rows, width = sizes
    me_grp = lax.axis_index("grp")
    me = lax.axis_index("dev")
    cores = 2
    chips = devs // cores
    chip, core = me // cores, lax.rem(me, cores)
    base = (me_grp * devs + me) * rows
    share = seeds // devs
    pieces = load_sem.shape[0]
    piece = rows // pieces
    tail = rounds - groups

    def load(k):
        return pltpu.make_async_copy(
            emb_hbm.at[pl.ds(k * piece, piece)], emb.at[pl.ds(k * piece, piece)], load_sem.at[k]
        )

    def load_ids(slot):
        which = me_grp + groups * slot
        return pltpu.make_async_copy(
            ids_hbm.at[pl.ds(which, 1)], ids.at[pl.ds(slot, 1)], id_sem.at[slot]
        )

    load_ids(0).start()
    for k in range(pieces):
        load(k).start()
    load_prior = pltpu.make_async_copy(prior_hbm, prior, prior_sem)
    load_prior.start()

    @pl.when(me_grp < tail)
    def _():
        load_ids(1).start()

    barrier = pltpu.get_barrier_semaphore()

    @pl.loop(1, devs)
    def _(p):
        pl.semaphore_signal(barrier, inc=1, device_id={"dev": lax.rem(me + p, devs)}, device_id_type=MESH)

    for p in range(1, groups):
        pl.semaphore_signal(
            barrier, inc=1, device_id={"grp": lax.rem(me_grp + p, groups)}, device_id_type=MESH
        )

    for edge in (0, EDGE + 2 * rows):
        wide[pl.ds(edge, EDGE), :] = jnp.zeros((EDGE, LANES), jnp.float32)
    for k in range(pieces):
        load(k).wait()

        @pl.loop(0, piece // 128)
        def _(t, k=k):
            at = pl.multiple_of(k * piece + t * 128, 128)
            x = emb[pl.ds(at, 128), :].astype(jnp.float32)
            for h in range(2):
                wide[pl.ds(EDGE + 2 * at + h, 128, stride=2), :] = x[:, h * LANES : (h + 1) * LANES]

    def pick(slot):
        load_ids(slot).wait()

        @pl.loop(0, seeds // PICK)
        def _(t):
            for u in range(PICK):
                at = jnp.clip(ids[slot, t * PICK + u] - base, -1, rows)
                pick_wide[pl.ds(2 * (t * PICK + u), 2), :] = wide[pl.ds(2 * at + EDGE, 2), :]

        @pl.loop(0, devs, unroll=4)
        def _(t):
            for h in range(2):
                picks[slot, t, :, h * LANES : (h + 1) * LANES] = pick_wide[
                    pl.ds(2 * share * t + h, share, stride=2), :
                ].astype(jnp.bfloat16)

    def scatter(slot):
        @pl.loop(1, devs)
        def _(p):
            to = lax.rem(me + p, devs)
            pltpu.make_async_remote_copy(
                src_ref=picks.at[slot, to],
                dst_ref=parts.at[slot, me],
                send_sem=send_sem.at[slot],
                recv_sem=part_sem.at[slot],
                device_id={"dev": to},
                device_id_type=MESH,
            ).start()

        parts[slot, pl.ds(me, 1)] = picks[slot, pl.ds(me, 1)]

    def take(slot):
        arrived(parts.at[slot, pl.ds(0, devs - 1)], part_sem.at[slot])
        total = jnp.sum(parts[slot].astype(jnp.float32), axis=0)
        blocks[me_grp + groups * slot] = total.astype(jnp.bfloat16)

    def trade(slot):
        index = me_grp + groups * slot
        for p in range(1, groups):
            pltpu.make_async_remote_copy(
                src_ref=blocks.at[index],
                dst_ref=blocks.at[index],
                send_sem=send_sem.at[2 + slot],
                recv_sem=block_sem.at[slot],
                device_id={"grp": lax.rem(me_grp + p, groups)},
                device_id_type=MESH,
            ).start()

    def spread(r):
        @pl.loop(1, chips)
        def _(p):
            pltpu.make_async_remote_copy(
                src_ref=blocks.at[r],
                dst_ref=centers.at[r, core, chip],
                send_sem=send_sem.at[4 + r],
                recv_sem=center_sem.at[r],
                device_id={"dev": lax.rem(chip + p, chips) * cores + core},
                device_id_type=MESH,
            ).start()

        centers[r, core, chip] = blocks[r]

    def relay(r):
        arrived(centers.at[r, 0, pl.ds(0, chips - 1)], center_sem.at[r])
        pltpu.make_async_remote_copy(
            src_ref=centers.at[r, core],
            dst_ref=centers.at[r, core],
            send_sem=send_sem.at[4 + rounds + r],
            recv_sem=relay_sem.at[r],
            device_id={"dev": chip * cores + 1 - core},
            device_id_type=MESH,
        ).start()

    def turn(i):
        lap = i // groups
        return lap * groups + lax.rem(me_grp * (1 - lap) + i, groups)

    pick(0)
    pl.semaphore_wait(barrier, devs - 1 + groups - 1)
    scatter(0)
    row_norms(emb, norms, accs)

    @pl.when(me_grp < tail)
    def _():
        pick(1)

    take(0)
    trade(0)
    spread(me_grp)

    @pl.when(me_grp < tail)
    def _():
        scatter(1)

    arrived(blocks.at[pl.ds(0, groups - 1)], block_sem.at[0])
    for i in range(1, groups):
        spread(turn(i))
    push_tiles(emb, 0)

    @pl.loop(0, rounds)
    def _(i):
        r = turn(i)
        relay(r)

        @pl.when((i == 1) & (me_grp < tail))
        def _():
            take(1)
            trade(1)

        @pl.when(i == 2)
        def _():
            @pl.when(me_grp < tail)
            def _():
                arrived(blocks.at[pl.ds(0, tail - 1)], block_sem.at[1])

            @pl.when(me_grp >= tail)
            def _():
                arrived(blocks.at[pl.ds(0, tail)], block_sem.at[1])

            for s in range(groups, rounds):
                spread(s)

        def between():
            arrived(centers.at[r, 0], relay_sem.at[r])

        sides = (centers.at[r, core], centers.at[r, 1 - core])
        nearest_of(emb, sides, half, best, accs, between)
        nearest[r] = jnp.maximum(norms[...] - 2.0 * best[...], 0.0) / float(width)

    for q in range(2):
        unused = accs[q][PIECES]
        pltpu.matmul_acc_lhs(unused, jnp.zeros((NORM_ROWS, width), jnp.bfloat16), load_staged_rhs=0)
        pltpu.matmul_pop(unused)

    load_prior.wait()
    current = prior[...]
    own_rows[...] = jnp.zeros((8, LANES), jnp.float32)
    for r in range(rounds):
        current = jnp.minimum(current, nearest[r])
        own_rows[pl.ds(r, 1), :] = jnp.sum(current, axis=0, keepdims=True)
    both_ref[pl.ds(0, rows // LANES), :] = current
    sums = jnp.broadcast_to(jnp.sum(own_rows[...], axis=1, keepdims=True), (8, LANES))
    lane = lax.broadcasted_iota(jnp.int32, (8, LANES), 1)
    row = lax.broadcasted_iota(jnp.int32, (8, LANES), 0)
    own_total[...] = jnp.sum(jnp.where(lane == row, sums, 0.0), axis=0, keepdims=True)

    @pl.loop(1, devs)
    def _(p):
        pltpu.make_async_remote_copy(
            src_ref=own_total,
            dst_ref=totals.at[me],
            send_sem=send_sem.at[4 + 2 * rounds],
            recv_sem=total_sem,
            device_id={"dev": lax.rem(me + p, devs)},
            device_id_type=MESH,
        ).start()

    totals[pl.ds(me, 1)] = own_total[...][None]
    arrived(totals.at[pl.ds(0, devs - 1)], total_sem)
    mean = jnp.sum(totals[...], axis=0) / float(rows * devs)
    both_ref[pl.ds(rows // LANES, 8), :] = jnp.broadcast_to(mean, (8, LANES))

    arrived(parts.at[0, pl.ds(0, devs - 1)], send_sem.at[0])
    arrived(blocks.at[pl.ds(0, groups - 1)], send_sem.at[2])

    @pl.when(me_grp < tail)
    def _():
        arrived(parts.at[1, pl.ds(0, devs - 1)], send_sem.at[1])
        arrived(blocks.at[pl.ds(0, groups - 1)], send_sem.at[3])

    for r in range(rounds):
        arrived(centers.at[r, 0, pl.ds(0, chips - 1)], send_sem.at[4 + r])
        arrived(centers.at[r, 0], send_sem.at[4 + rounds + r])
    arrived(totals.at[pl.ds(0, devs - 1)], send_sem.at[4 + 2 * rounds])


def finish(both, dist_ref, mean_ref):
    count = dist_ref.shape[0]
    dist_ref[...] = both[pl.ds(0, count), :]
    mean_ref[...] = both[pl.ds(count, 1), : mean_ref.shape[1]]


def body(embeddings, prior_dist, seed_ids):
    rows, width = embeddings.shape
    rounds, seeds = seed_ids.shape
    groups, devs = lax.axis_size("grp"), lax.axis_size("dev")
    share = seeds // devs
    slots = -(-rounds // groups)
    sizes = (groups, devs, rounds, seeds, rows, width)
    flat = (rows // LANES, LANES)
    vmem = pl.BlockSpec(memory_space=pltpu.VMEM)
    hbm = pl.BlockSpec(memory_space=pltpu.HBM)
    inputs = (seed_ids, embeddings, prior_dist.reshape(flat))
    both = pl.pallas_call(
        functools.partial(kernel, sizes),
        name="seeding",
        out_shape=jax.ShapeDtypeStruct((rows // LANES + 8, LANES), jnp.float32),
        in_specs=[hbm, hbm, hbm],
        out_specs=vmem,
        scratch_shapes=[
            pltpu.SMEM((slots, seeds), jnp.int32),
            pltpu.VMEM((rows, width), jnp.bfloat16),
            pltpu.VMEM(flat, jnp.float32),
            pltpu.VMEM((2 * rows + 2 * EDGE, LANES), jnp.float32),
            pltpu.VMEM((2 * seeds, LANES), jnp.float32),
            pltpu.VMEM((slots, devs, share, width), jnp.bfloat16),
            pltpu.VMEM((slots, devs, share, width), jnp.bfloat16),
            pltpu.VMEM((rounds, share, width), jnp.bfloat16),
            pltpu.VMEM((rounds, 2, devs // 2, share, width), jnp.bfloat16),
            pltpu.VMEM((2, seeds // 2, LANES), jnp.float32),
            pltpu.VMEM(flat, jnp.float32),
            pltpu.VMEM(flat, jnp.float32),
            pltpu.VMEM((rounds, *flat), jnp.float32),
            pltpu.VMEM((8, LANES), jnp.float32),
            pltpu.VMEM((1, LANES), jnp.float32),
            pltpu.VMEM((devs, 1, LANES), jnp.float32),
            pltpu.SemaphoreType.DMA((8,)),
            pltpu.SemaphoreType.DMA((slots,)),
            pltpu.SemaphoreType.DMA,
            pltpu.SemaphoreType.DMA((5 + 2 * rounds,)),
            pltpu.SemaphoreType.DMA((2,)),
            pltpu.SemaphoreType.DMA((2,)),
            pltpu.SemaphoreType.DMA((rounds,)),
            pltpu.SemaphoreType.DMA((rounds,)),
            pltpu.SemaphoreType.DMA,
        ],
        compiler_params=pltpu.CompilerParams(
            collective_id=0, has_side_effects=True, vmem_limit_bytes=48 * 1024 * 1024
        ),
    )(*(pltpu.with_memory_space_constraint(x, pltpu.HBM) for x in inputs))
    dist, means = pl.pallas_call(
        finish,
        name="finish",
        out_shape=(
            jax.ShapeDtypeStruct(flat, jnp.float32),
            jax.ShapeDtypeStruct((1, rounds), jnp.float32),
        ),
        in_specs=[vmem],
        out_specs=(vmem, vmem),
        compiler_params=pltpu.CompilerParams(vmem_limit_bytes=1024 * 1024),
    )(both)
    return dist.reshape(rows), means.reshape(rounds, 1)


def solution(mesh):
    placed = (P(("grp", "dev"), None), P(("grp", "dev")), P())
    return jax.shard_map(
        body,
        mesh=mesh,
        in_specs=placed,
        out_specs=(P(("grp", "dev")), P(None, "grp")),
        check_vma=False,
    )
```

```python
import functools

import jax
import jax.numpy as jnp
from jax import lax
from jax.experimental import pallas as pl
from jax.experimental.pallas import tpu as pltpu
from jax.sharding import PartitionSpec as P

MESH = pl.DeviceIdType.MESH
PICK = 32
CHUNK = 256
LANES = 128
PIECE = 128
PIECES = 7
LAG = 4
EDGE = 8
NORM_ROWS = 16
NORM_PARTS = 2


def tile_of(emb, j):
    return emb[pl.ds(pl.multiple_of(j * CHUNK, CHUNK), CHUNK), :]


def row_norms(emb, norms, accs, part):
    width = emb.shape[1]
    ones = jnp.ones((NORM_ROWS, width), jnp.bfloat16)
    steps = 4

    trips = emb.shape[0] // CHUNK // (2 * steps)

    @pl.loop(part * trips // NORM_PARTS, (part + 1) * trips // NORM_PARTS)
    def _(t):
        for i in range(steps):
            for q in range(2):
                j = (t * steps + i) * 2 + q
                x = tile_of(emb, j).astype(jnp.float32)
                square = x * x
                high = square.astype(jnp.bfloat16)
                low = (square - high.astype(jnp.float32)).astype(jnp.bfloat16)
                acc = accs[q][PIECES + i]
                for part in (high, low):
                    pltpu.matmul_push_rhs(part, staging_register=0, mxu_index=q, transpose=True)
                    pltpu.matmul_acc_lhs(acc, ones, load_staged_rhs=0)
                total = pltpu.matmul_pop(acc)
                for k in range(CHUNK // LANES):
                    norms[pl.ds(j * (CHUNK // LANES) + k, 1), :] = total[
                        0:1, k * LANES : (k + 1) * LANES
                    ]


def push_tiles(emb, t):
    for q in range(2):
        pltpu.matmul_push_rhs(
            tile_of(emb, t * 2 + q), staging_register=0, mxu_index=q, transpose=True
        )


def half_norms(center, half, unit):
    chips, share, width = center.shape
    wide_c = center[...].reshape(chips * share, width).astype(jnp.float32)
    half[unit] = jnp.broadcast_to(
        0.5 * jnp.sum(wide_c * wide_c, axis=1, keepdims=True), (chips * share, LANES)
    )


def nearest_of(emb, sides, half, best, accs, between):
    chips, share, width = sides[0].shape
    trips = emb.shape[0] // CHUNK // 2
    pieces = chips * share // PIECE
    pending = []
    run = {}

    def pop():
        unit, t, p, use = pending.pop(0)
        offset = half[unit, pl.ds(p * PIECE, PIECE), :]
        for q in range(2):
            value = pltpu.matmul_pop(use[q])
            for k in range(CHUNK // LANES):
                short = value[:, k * LANES : (k + 1) * LANES] - offset
                short = jnp.max(short.reshape(PIECE // 8, 8, LANES), axis=0)
                run[q, k] = jnp.maximum(run[q, k], short) if p else short
        if p == pieces - 1:
            for (q, k), value in list(run.items()):
                row = (t * 2 + q) * (CHUNK // LANES) + k
                value = jnp.max(value, axis=0, keepdims=True)
                if unit:
                    value = jnp.maximum(value, best[pl.ds(row, 1), :])
                best[pl.ds(row, 1), :] = value

    count = 0
    for unit in range(2):
        if unit:
            between()
        half_norms(sides[unit], half, unit)
        for t in range(trips):
            for p in range(pieces):
                lhs = sides[unit][pl.ds(p * PIECE // share, PIECE // share)].reshape(PIECE, width)
                use = [accs[q][count % PIECES] for q in range(2)]
                count += 1
                for q in range(2):
                    pltpu.matmul_acc_lhs(use[q], lhs, load_staged_rhs=None if p else 0)
                if p == 0:
                    push_tiles(emb, (t + 1) % trips)
                pending.append((unit, t, p, use))
                if len(pending) > LAG:
                    pop()
    while pending:
        pop()


def kernel(sizes, *refs):
    specs = [
        pltpu.ACC(q)((rows, CHUNK), jnp.float32)
        for q in range(2)
        for rows in [PIECE] * PIECES + [NORM_ROWS] * 4
    ]

    def inner(*accs):
        half = len(accs) // 2
        run_kernel(sizes, *refs, (accs[:half], accs[half:]))

    pl.run_scoped(inner, *specs)


def arrived(ref, sem):
    pltpu.make_async_copy(ref, ref, sem).wait()


def run_kernel(
    sizes,
    ids_hbm,
    emb_hbm,
    prior_hbm,
    both_ref,
    ids,
    emb,
    prior,
    wide,
    pick_wide,
    picks,
    parts,
    blocks,
    centers,
    half,
    norms,
    best,
    nearest,
    own_rows,
    own_total,
    totals,
    load_sem,
    id_sem,
    prior_sem,
    send_sem,
    part_sem,
    block_sem,
    center_sem,
    relay_sem,
    total_sem,
    accs,
):
    groups, devs, rounds, seeds, rows, width = sizes
    me_grp = lax.axis_index("grp")
    me = lax.axis_index("dev")
    cores = 2
    chips = devs // cores
    chip, core = me // cores, lax.rem(me, cores)
    base = (me_grp * devs + me) * rows
    share = seeds // devs
    pieces = load_sem.shape[0]
    piece = rows // pieces
    tail = rounds - groups
    reach = (1, 3, 2)

    def load(k):
        return pltpu.make_async_copy(
            emb_hbm.at[pl.ds(k * piece, piece)], emb.at[pl.ds(k * piece, piece)], load_sem.at[k]
        )

    def load_ids(slot):
        which = me_grp + groups * slot
        return pltpu.make_async_copy(
            ids_hbm.at[pl.ds(which, 1)], ids.at[pl.ds(slot, 1)], id_sem.at[slot]
        )

    load_ids(0).start()
    for k in range(pieces):
        load(k).start()
    load_prior = pltpu.make_async_copy(prior_hbm, prior, prior_sem)
    load_prior.start()

    @pl.when(me_grp < tail)
    def _():
        load_ids(1).start()

    barrier = pltpu.get_barrier_semaphore()

    @pl.loop(1, devs)
    def _(p):
        pl.semaphore_signal(barrier, inc=1, device_id={"dev": lax.rem(me + p, devs)}, device_id_type=MESH)

    for p in range(1, groups):
        pl.semaphore_signal(
            barrier, inc=1, device_id={"grp": lax.rem(me_grp + p, groups)}, device_id_type=MESH
        )

    for edge in (0, EDGE + 2 * rows):
        wide[pl.ds(edge, EDGE), :] = jnp.zeros((EDGE, LANES), jnp.float32)
    for k in range(pieces):
        load(k).wait()

        @pl.loop(0, piece // 128)
        def _(t, k=k):
            at = pl.multiple_of(k * piece + t * 128, 128)
            x = emb[pl.ds(at, 128), :].astype(jnp.float32)
            for h in range(2):
                wide[pl.ds(EDGE + 2 * at + h, 128, stride=2), :] = x[:, h * LANES : (h + 1) * LANES]

    def owner(q):
        return lax.rem(me + 1 + q, devs)

    def pick(slot, t):
        for v in range(PICK // share):
            to = owner(t * (PICK // share) + v)
            row = pl.multiple_of(to * 2 * share, 2 * share)
            for u in range(share):
                at = jnp.clip(ids[slot, to * share + u] - base, -1, rows)
                pick_wide[pl.ds(row + 2 * u, 2), :] = wide[pl.ds(2 * at + EDGE, 2), :]
            for h in range(2):
                picks[slot, to, :, h * LANES : (h + 1) * LANES] = pick_wide[
                    pl.ds(row + h, share, stride=2), :
                ].astype(jnp.bfloat16)

    def send_pick(slot, q):
        to = owner(q)
        pltpu.make_async_remote_copy(
            src_ref=picks.at[slot, to],
            dst_ref=parts.at[slot, me],
            send_sem=send_sem.at[slot],
            recv_sem=part_sem.at[slot],
            device_id={"dev": to},
            device_id_type=MESH,
        ).start()

    def scatter(slot, entry=None):
        load_ids(slot).wait()
        each = PICK // share
        pick(slot, 0)
        if entry is not None:
            entry()

        @pl.loop(1, devs // each)
        def _(t):
            pick(slot, t)
            for v in range(each):
                send_pick(slot, (t - 1) * each + v)

        for q in range(devs - each, devs - 1):
            send_pick(slot, q)
        parts[slot, pl.ds(me, 1)] = picks[slot, pl.ds(me, 1)]

    def take(slot):
        arrived(parts.at[slot, pl.ds(0, devs - 1)], part_sem.at[slot])
        total = jnp.sum(parts[slot].astype(jnp.float32), axis=0)
        blocks[me_grp + groups * slot] = total.astype(jnp.bfloat16)

    def trade(slot):
        index = me_grp + groups * slot
        for p in reach:
            pltpu.make_async_remote_copy(
                src_ref=blocks.at[index],
                dst_ref=blocks.at[index],
                send_sem=send_sem.at[2 + slot],
                recv_sem=block_sem.at[index],
                device_id={"grp": lax.rem(me_grp + p, groups)},
                device_id_type=MESH,
            ).start()

    def spread(r):
        @pl.loop(1, chips)
        def _(p):
            pltpu.make_async_remote_copy(
                src_ref=blocks.at[r],
                dst_ref=centers.at[r, core, chip],
                send_sem=send_sem.at[4 + r],
                recv_sem=center_sem.at[r],
                device_id={"dev": lax.rem(chip + p, chips) * cores + core},
                device_id_type=MESH,
            ).start()

        centers[r, core, chip] = blocks[r]

    def relay(r):
        arrived(centers.at[r, 0, pl.ds(0, chips - 1)], center_sem.at[r])
        pltpu.make_async_remote_copy(
            src_ref=centers.at[r, core],
            dst_ref=centers.at[r, core],
            send_sem=send_sem.at[4 + rounds + r],
            recv_sem=relay_sem.at[r],
            device_id={"dev": chip * cores + 1 - core},
            device_id_type=MESH,
        ).start()

    def turn(i):
        lap, j = i // groups, lax.rem(i, groups)
        ahead = j + j // 2 * (groups + 1 - 2 * j)
        return lap * groups + lax.rem(me_grp * (1 - lap) + ahead, groups)

    scatter(0, lambda: pl.semaphore_wait(barrier, devs - 1 + groups - 1))

    @pl.when(me_grp < tail)
    def _():
        scatter(1)

    row_norms(emb, norms, accs, 0)
    take(0)
    trade(0)
    spread(me_grp)

    row_norms(emb, norms, accs, 1)
    for p in reach:
        near = lax.rem(me_grp + p, groups)
        arrived(blocks.at[near], block_sem.at[near])
        spread(near)
    push_tiles(emb, 0)

    @pl.loop(0, rounds)
    def _(i):
        r = turn(i)
        relay(r)

        @pl.when((i == 1) & (me_grp < tail))
        def _():
            take(1)
            trade(1)

        @pl.when(i == 2)
        def _():
            for index in range(groups, rounds):

                @pl.when(me_grp != index - groups)
                def _():
                    arrived(blocks.at[index], block_sem.at[index])

                spread(index)

        def between():
            arrived(centers.at[r, 0], relay_sem.at[r])

        sides = (centers.at[r, core], centers.at[r, 1 - core])
        nearest_of(emb, sides, half, best, accs, between)
        nearest[r] = jnp.maximum(norms[...] - 2.0 * best[...], 0.0) / float(width)

    for q in range(2):
        unused = accs[q][PIECES]
        pltpu.matmul_acc_lhs(unused, jnp.zeros((NORM_ROWS, width), jnp.bfloat16), load_staged_rhs=0)
        pltpu.matmul_pop(unused)

    load_prior.wait()
    current = prior[...]
    own_rows[...] = jnp.zeros((8, LANES), jnp.float32)
    for r in range(rounds):
        current = jnp.minimum(current, nearest[r])
        own_rows[pl.ds(r, 1), :] = jnp.sum(current, axis=0, keepdims=True)
    both_ref[pl.ds(0, rows // LANES), :] = current
    sums = jnp.broadcast_to(jnp.sum(own_rows[...], axis=1, keepdims=True), (8, LANES))
    lane = lax.broadcasted_iota(jnp.int32, (8, LANES), 1)
    row = lax.broadcasted_iota(jnp.int32, (8, LANES), 0)
    own_total[...] = jnp.sum(jnp.where(lane == row, sums, 0.0), axis=0, keepdims=True)

    @pl.loop(1, devs)
    def _(p):
        pltpu.make_async_remote_copy(
            src_ref=own_total,
            dst_ref=totals.at[me],
            send_sem=send_sem.at[4 + 2 * rounds],
            recv_sem=total_sem,
            device_id={"dev": lax.rem(me + p, devs)},
            device_id_type=MESH,
        ).start()

    totals[pl.ds(me, 1)] = own_total[...][None]
    arrived(totals.at[pl.ds(0, devs - 1)], total_sem)
    mean = jnp.sum(totals[...], axis=0) / float(rows * devs)
    both_ref[pl.ds(rows // LANES, 8), :] = jnp.broadcast_to(mean, (8, LANES))

    arrived(parts.at[0, pl.ds(0, devs - 1)], send_sem.at[0])
    arrived(blocks.at[pl.ds(0, groups - 1)], send_sem.at[2])

    @pl.when(me_grp < tail)
    def _():
        arrived(parts.at[1, pl.ds(0, devs - 1)], send_sem.at[1])
        arrived(blocks.at[pl.ds(0, groups - 1)], send_sem.at[3])

    for r in range(rounds):
        arrived(centers.at[r, 0, pl.ds(0, chips - 1)], send_sem.at[4 + r])
        arrived(centers.at[r, 0], send_sem.at[4 + rounds + r])
    arrived(totals.at[pl.ds(0, devs - 1)], send_sem.at[4 + 2 * rounds])


def finish(both, dist_ref, mean_ref):
    count = dist_ref.shape[0]
    dist_ref[...] = both[pl.ds(0, count), :]
    mean_ref[...] = both[pl.ds(count, 1), : mean_ref.shape[1]]


def body(embeddings, prior_dist, seed_ids):
    rows, width = embeddings.shape
    rounds, seeds = seed_ids.shape
    groups, devs = lax.axis_size("grp"), lax.axis_size("dev")
    share = seeds // devs
    slots = -(-rounds // groups)
    sizes = (groups, devs, rounds, seeds, rows, width)
    flat = (rows // LANES, LANES)
    vmem = pl.BlockSpec(memory_space=pltpu.VMEM)
    hbm = pl.BlockSpec(memory_space=pltpu.HBM)
    inputs = (seed_ids, embeddings, prior_dist.reshape(flat))
    both = pl.pallas_call(
        functools.partial(kernel, sizes),
        name="seeding",
        out_shape=jax.ShapeDtypeStruct((rows // LANES + 8, LANES), jnp.float32),
        in_specs=[hbm, hbm, hbm],
        out_specs=vmem,
        scratch_shapes=[
            pltpu.SMEM((slots, seeds), jnp.int32),
            pltpu.VMEM((rows, width), jnp.bfloat16),
            pltpu.VMEM(flat, jnp.float32),
            pltpu.VMEM((2 * rows + 2 * EDGE, LANES), jnp.float32),
            pltpu.VMEM((2 * seeds, LANES), jnp.float32),
            pltpu.VMEM((slots, devs, share, width), jnp.bfloat16),
            pltpu.VMEM((slots, devs, share, width), jnp.bfloat16),
            pltpu.VMEM((rounds, share, width), jnp.bfloat16),
            pltpu.VMEM((rounds, 2, devs // 2, share, width), jnp.bfloat16),
            pltpu.VMEM((2, seeds // 2, LANES), jnp.float32),
            pltpu.VMEM(flat, jnp.float32),
            pltpu.VMEM(flat, jnp.float32),
            pltpu.VMEM((rounds, *flat), jnp.float32),
            pltpu.VMEM((8, LANES), jnp.float32),
            pltpu.VMEM((1, LANES), jnp.float32),
            pltpu.VMEM((devs, 1, LANES), jnp.float32),
            pltpu.SemaphoreType.DMA((8,)),
            pltpu.SemaphoreType.DMA((slots,)),
            pltpu.SemaphoreType.DMA,
            pltpu.SemaphoreType.DMA((5 + 2 * rounds,)),
            pltpu.SemaphoreType.DMA((2,)),
            pltpu.SemaphoreType.DMA((rounds,)),
            pltpu.SemaphoreType.DMA((rounds,)),
            pltpu.SemaphoreType.DMA((rounds,)),
            pltpu.SemaphoreType.DMA,
        ],
        compiler_params=pltpu.CompilerParams(
            collective_id=0, has_side_effects=True, vmem_limit_bytes=48 * 1024 * 1024
        ),
    )(*(pltpu.with_memory_space_constraint(x, pltpu.HBM) for x in inputs))
    dist, means = pl.pallas_call(
        finish,
        name="finish",
        out_shape=(
            jax.ShapeDtypeStruct(flat, jnp.float32),
            jax.ShapeDtypeStruct((1, rounds), jnp.float32),
        ),
        in_specs=[vmem],
        out_specs=(vmem, vmem),
        compiler_params=pltpu.CompilerParams(vmem_limit_bytes=1024 * 1024),
    )(both)
    return dist.reshape(rows), means.reshape(rounds, 1)


def solution(mesh):
    placed = (P(("grp", "dev"), None), P(("grp", "dev")), P())
    return jax.shard_map(
        body,
        mesh=mesh,
        in_specs=placed,
        out_specs=(P(("grp", "dev")), P(None, "grp")),
        check_vma=False,
    )
```

```python
import functools

import jax
import jax.numpy as jnp
from jax import lax
from jax.experimental import pallas as pl
from jax.experimental.pallas import tpu as pltpu
from jax.sharding import PartitionSpec as P

MESH = pl.DeviceIdType.MESH
PICK = 32
CHUNK = 256
LANES = 128
PIECE = 128
PIECES = 7
LAG = 4
EDGE = 8
NORM_ROWS = 16
NORM_PARTS = 2


def tile_of(emb, j):
    return emb[pl.ds(pl.multiple_of(j * CHUNK, CHUNK), CHUNK), :]


def row_norms(emb, norms, accs, part):
    width = emb.shape[1]
    ones = jnp.ones((NORM_ROWS, width), jnp.bfloat16)
    steps = 4

    trips = emb.shape[0] // CHUNK // (2 * steps)

    @pl.loop(part * trips // NORM_PARTS, (part + 1) * trips // NORM_PARTS)
    def _(t):
        for i in range(steps):
            for q in range(2):
                j = (t * steps + i) * 2 + q
                x = tile_of(emb, j).astype(jnp.float32)
                square = x * x
                high = square.astype(jnp.bfloat16)
                low = (square - high.astype(jnp.float32)).astype(jnp.bfloat16)
                acc = accs[q][PIECES + i]
                for part in (high, low):
                    pltpu.matmul_push_rhs(part, staging_register=0, mxu_index=q, transpose=True)
                    pltpu.matmul_acc_lhs(acc, ones, load_staged_rhs=0)
                total = pltpu.matmul_pop(acc)
                for k in range(CHUNK // LANES):
                    norms[pl.ds(j * (CHUNK // LANES) + k, 1), :] = total[
                        0:1, k * LANES : (k + 1) * LANES
                    ]


def push_tiles(emb, t):
    for q in range(2):
        pltpu.matmul_push_rhs(
            tile_of(emb, t * 2 + q), staging_register=0, mxu_index=q, transpose=True
        )


def half_norms(center, half, unit):
    chips, share, width = center.shape
    wide_c = center[...].reshape(chips * share, width).astype(jnp.float32)
    half[unit] = jnp.broadcast_to(
        0.5 * jnp.sum(wide_c * wide_c, axis=1, keepdims=True), (chips * share, LANES)
    )


def nearest_of(emb, sides, half, best, accs, between):
    chips, share, width = sides[0].shape
    trips = emb.shape[0] // CHUNK // 2
    pieces = chips * share // PIECE
    pending = []
    run = {}

    def pop():
        unit, t, p, use = pending.pop(0)
        offset = half[unit, pl.ds(p * PIECE, PIECE), :]
        for q in range(2):
            value = pltpu.matmul_pop(use[q])
            for k in range(CHUNK // LANES):
                short = value[:, k * LANES : (k + 1) * LANES] - offset
                short = jnp.max(short.reshape(PIECE // 8, 8, LANES), axis=0)
                run[q, k] = jnp.maximum(run[q, k], short) if p else short
        if p == pieces - 1:
            for (q, k), value in list(run.items()):
                row = (t * 2 + q) * (CHUNK // LANES) + k
                value = jnp.max(value, axis=0, keepdims=True)
                if unit:
                    value = jnp.maximum(value, best[pl.ds(row, 1), :])
                best[pl.ds(row, 1), :] = value

    count = 0
    for unit in range(2):
        if unit:
            between()
        half_norms(sides[unit], half, unit)
        for t in range(trips):
            for p in range(pieces):
                lhs = sides[unit][pl.ds(p * PIECE // share, PIECE // share)].reshape(PIECE, width)
                use = [accs[q][count % PIECES] for q in range(2)]
                count += 1
                for q in range(2):
                    pltpu.matmul_acc_lhs(use[q], lhs, load_staged_rhs=None if p else 0)
                if p == 0:
                    push_tiles(emb, (t + 1) % trips)
                pending.append((unit, t, p, use))
                if len(pending) > LAG:
                    pop()
    while pending:
        pop()


def kernel(sizes, *refs):
    specs = [
        pltpu.ACC(q)((rows, CHUNK), jnp.float32)
        for q in range(2)
        for rows in [PIECE] * PIECES + [NORM_ROWS] * 4
    ]

    def inner(*accs):
        half = len(accs) // 2
        run_kernel(sizes, *refs, (accs[:half], accs[half:]))

    pl.run_scoped(inner, *specs)


def arrived(ref, sem):
    pltpu.make_async_copy(ref, ref, sem).wait()


def run_kernel(
    sizes,
    ids_hbm,
    emb_hbm,
    prior_hbm,
    both_ref,
    ids,
    emb,
    prior,
    wide,
    pick_wide,
    picks,
    parts,
    blocks,
    centers,
    half,
    norms,
    best,
    nearest,
    own_rows,
    own_total,
    totals,
    load_sem,
    id_sem,
    prior_sem,
    send_sem,
    part_sem,
    block_sem,
    center_sem,
    relay_sem,
    total_sem,
    accs,
):
    groups, devs, rounds, seeds, rows, width = sizes
    me_grp = lax.axis_index("grp")
    me = lax.axis_index("dev")
    cores = 2
    chips = devs // cores
    chip, core = me // cores, lax.rem(me, cores)
    base = (me_grp * devs + me) * rows
    share = seeds // devs
    pieces = load_sem.shape[0]
    piece = rows // pieces
    tail = rounds - groups
    reach = (1, 3, 2)

    def load(k):
        return pltpu.make_async_copy(
            emb_hbm.at[pl.ds(k * piece, piece)], emb.at[pl.ds(k * piece, piece)], load_sem.at[k]
        )

    def load_ids(slot):
        which = me_grp + groups * slot
        return pltpu.make_async_copy(
            ids_hbm.at[pl.ds(which, 1)], ids.at[pl.ds(slot, 1)], id_sem.at[slot]
        )

    load_ids(0).start()
    for k in range(pieces):
        load(k).start()
    load_prior = pltpu.make_async_copy(prior_hbm, prior, prior_sem)
    load_prior.start()

    @pl.when(me_grp < tail)
    def _():
        load_ids(1).start()

    barrier = pltpu.get_barrier_semaphore()

    @pl.loop(1, devs)
    def _(p):
        pl.semaphore_signal(barrier, inc=1, device_id={"dev": lax.rem(me + p, devs)}, device_id_type=MESH)

    for p in range(1, groups):
        pl.semaphore_signal(
            barrier, inc=1, device_id={"grp": lax.rem(me_grp + p, groups)}, device_id_type=MESH
        )

    for edge in (0, EDGE + 2 * rows):
        wide[pl.ds(edge, EDGE), :] = jnp.zeros((EDGE, LANES), jnp.float32)
    for k in range(pieces):
        load(k).wait()

        @pl.loop(0, piece // 128)
        def _(t, k=k):
            at = pl.multiple_of(k * piece + t * 128, 128)
            x = emb[pl.ds(at, 128), :].astype(jnp.float32)
            for h in range(2):
                wide[pl.ds(EDGE + 2 * at + h, 128, stride=2), :] = x[:, h * LANES : (h + 1) * LANES]

    def owner(q):
        return lax.rem(me + 1 + q, devs)

    def pick(slot, t):
        for v in range(PICK // share):
            to = owner(t * (PICK // share) + v)
            row = pl.multiple_of(to * 2 * share, 2 * share)
            for u in range(share):
                at = jnp.clip(ids[slot, to * share + u] - base, -1, rows)
                pick_wide[pl.ds(row + 2 * u, 2), :] = wide[pl.ds(2 * at + EDGE, 2), :]
            for h in range(2):
                picks[slot, to, :, h * LANES : (h + 1) * LANES] = pick_wide[
                    pl.ds(row + h, share, stride=2), :
                ].astype(jnp.bfloat16)

    def send_pick(slot, q):
        to = owner(q)
        pltpu.make_async_remote_copy(
            src_ref=picks.at[slot, to],
            dst_ref=parts.at[slot, me],
            send_sem=send_sem.at[slot],
            recv_sem=part_sem.at[slot],
            device_id={"dev": to},
            device_id_type=MESH,
        ).start()

    def scatter(slot, entry=None):
        load_ids(slot).wait()
        each = PICK // share
        pick(slot, 0)
        if entry is not None:
            entry()

        @pl.loop(1, devs // each)
        def _(t):
            pick(slot, t)
            for v in range(each):
                send_pick(slot, (t - 1) * each + v)

        for q in range(devs - each, devs - 1):
            send_pick(slot, q)
        parts[slot, pl.ds(me, 1)] = picks[slot, pl.ds(me, 1)]

    def take(slot):
        arrived(parts.at[slot, pl.ds(0, devs - 1)], part_sem.at[slot])
        total = jnp.sum(parts[slot].astype(jnp.float32), axis=0)
        blocks[me_grp + groups * slot] = total.astype(jnp.bfloat16)

    def trade(slot):
        index = me_grp + groups * slot
        for p in reach:
            pltpu.make_async_remote_copy(
                src_ref=blocks.at[index],
                dst_ref=blocks.at[index],
                send_sem=send_sem.at[2 + slot],
                recv_sem=block_sem.at[index],
                device_id={"grp": lax.rem(me_grp + p, groups)},
                device_id_type=MESH,
            ).start()

    def spread(r):
        @pl.loop(1, chips)
        def _(p):
            pltpu.make_async_remote_copy(
                src_ref=blocks.at[r],
                dst_ref=centers.at[r, core, chip],
                send_sem=send_sem.at[4 + r],
                recv_sem=center_sem.at[r],
                device_id={"dev": lax.rem(chip + p, chips) * cores + core},
                device_id_type=MESH,
            ).start()

        centers[r, core, chip] = blocks[r]

    def relay(r):
        arrived(centers.at[r, 0, pl.ds(0, chips - 1)], center_sem.at[r])
        pltpu.make_async_remote_copy(
            src_ref=centers.at[r, core],
            dst_ref=centers.at[r, core],
            send_sem=send_sem.at[4 + rounds + r],
            recv_sem=relay_sem.at[r],
            device_id={"dev": chip * cores + 1 - core},
            device_id_type=MESH,
        ).start()

    def turn(i):
        lap, j = i // groups, lax.rem(i, groups)
        ahead = j + j // 2 * (groups + 1 - 2 * j)
        return lap * groups + lax.rem(me_grp * (1 - lap) + ahead, groups)

    scatter(0, lambda: pl.semaphore_wait(barrier, devs - 1 + groups - 1))

    @pl.when(me_grp < tail)
    def _():
        scatter(1)

    row_norms(emb, norms, accs, 0)
    take(0)
    trade(0)
    spread(me_grp)

    row_norms(emb, norms, accs, 1)
    for p in reach:
        near = lax.rem(me_grp + p, groups)
        arrived(blocks.at[near], block_sem.at[near])
        spread(near)

    @pl.when(me_grp < tail)
    def _():
        take(1)
        trade(1)

    push_tiles(emb, 0)

    @pl.loop(0, rounds)
    def _(i):
        r = turn(i)
        relay(r)

        @pl.when(i == 1)
        def _():
            for index in range(groups, rounds):

                @pl.when(me_grp != index - groups)
                def _():
                    arrived(blocks.at[index], block_sem.at[index])

                spread(index)

        def between():
            arrived(centers.at[r, 0], relay_sem.at[r])

        sides = (centers.at[r, core], centers.at[r, 1 - core])
        nearest_of(emb, sides, half, best, accs, between)
        nearest[r] = jnp.maximum(norms[...] - 2.0 * best[...], 0.0) / float(width)

    for q in range(2):
        unused = accs[q][PIECES]
        pltpu.matmul_acc_lhs(unused, jnp.zeros((NORM_ROWS, width), jnp.bfloat16), load_staged_rhs=0)
        pltpu.matmul_pop(unused)

    load_prior.wait()
    current = prior[...]
    own_rows[...] = jnp.zeros((8, LANES), jnp.float32)
    for r in range(rounds):
        current = jnp.minimum(current, nearest[r])
        own_rows[pl.ds(r, 1), :] = jnp.sum(current, axis=0, keepdims=True)
    both_ref[pl.ds(0, rows // LANES), :] = current
    sums = jnp.broadcast_to(jnp.sum(own_rows[...], axis=1, keepdims=True), (8, LANES))
    lane = lax.broadcasted_iota(jnp.int32, (8, LANES), 1)
    row = lax.broadcasted_iota(jnp.int32, (8, LANES), 0)
    own_total[...] = jnp.sum(jnp.where(lane == row, sums, 0.0), axis=0, keepdims=True)

    @pl.loop(1, devs)
    def _(p):
        pltpu.make_async_remote_copy(
            src_ref=own_total,
            dst_ref=totals.at[me],
            send_sem=send_sem.at[4 + 2 * rounds],
            recv_sem=total_sem,
            device_id={"dev": lax.rem(me + p, devs)},
            device_id_type=MESH,
        ).start()

    totals[pl.ds(me, 1)] = own_total[...][None]
    arrived(totals.at[pl.ds(0, devs - 1)], total_sem)
    mean = jnp.sum(totals[...], axis=0) / float(rows * devs)
    both_ref[pl.ds(rows // LANES, 8), :] = jnp.broadcast_to(mean, (8, LANES))

    arrived(parts.at[0, pl.ds(0, devs - 1)], send_sem.at[0])
    arrived(blocks.at[pl.ds(0, groups - 1)], send_sem.at[2])

    @pl.when(me_grp < tail)
    def _():
        arrived(parts.at[1, pl.ds(0, devs - 1)], send_sem.at[1])
        arrived(blocks.at[pl.ds(0, groups - 1)], send_sem.at[3])

    for r in range(rounds):
        arrived(centers.at[r, 0, pl.ds(0, chips - 1)], send_sem.at[4 + r])
        arrived(centers.at[r, 0], send_sem.at[4 + rounds + r])
    arrived(totals.at[pl.ds(0, devs - 1)], send_sem.at[4 + 2 * rounds])


def finish(both, dist_ref, mean_ref):
    count = dist_ref.shape[0]
    dist_ref[...] = both[pl.ds(0, count), :]
    mean_ref[...] = both[pl.ds(count, 1), : mean_ref.shape[1]]


def body(embeddings, prior_dist, seed_ids):
    rows, width = embeddings.shape
    rounds, seeds = seed_ids.shape
    groups, devs = lax.axis_size("grp"), lax.axis_size("dev")
    share = seeds // devs
    slots = -(-rounds // groups)
    sizes = (groups, devs, rounds, seeds, rows, width)
    flat = (rows // LANES, LANES)
    vmem = pl.BlockSpec(memory_space=pltpu.VMEM)
    hbm = pl.BlockSpec(memory_space=pltpu.HBM)
    inputs = (seed_ids, embeddings, prior_dist.reshape(flat))
    both = pl.pallas_call(
        functools.partial(kernel, sizes),
        name="seeding",
        out_shape=jax.ShapeDtypeStruct((rows // LANES + 8, LANES), jnp.float32),
        in_specs=[hbm, hbm, hbm],
        out_specs=vmem,
        scratch_shapes=[
            pltpu.SMEM((slots, seeds), jnp.int32),
            pltpu.VMEM((rows, width), jnp.bfloat16),
            pltpu.VMEM(flat, jnp.float32),
            pltpu.VMEM((2 * rows + 2 * EDGE, LANES), jnp.float32),
            pltpu.VMEM((2 * seeds, LANES), jnp.float32),
            pltpu.VMEM((slots, devs, share, width), jnp.bfloat16),
            pltpu.VMEM((slots, devs, share, width), jnp.bfloat16),
            pltpu.VMEM((rounds, share, width), jnp.bfloat16),
            pltpu.VMEM((rounds, 2, devs // 2, share, width), jnp.bfloat16),
            pltpu.VMEM((2, seeds // 2, LANES), jnp.float32),
            pltpu.VMEM(flat, jnp.float32),
            pltpu.VMEM(flat, jnp.float32),
            pltpu.VMEM((rounds, *flat), jnp.float32),
            pltpu.VMEM((8, LANES), jnp.float32),
            pltpu.VMEM((1, LANES), jnp.float32),
            pltpu.VMEM((devs, 1, LANES), jnp.float32),
            pltpu.SemaphoreType.DMA((8,)),
            pltpu.SemaphoreType.DMA((slots,)),
            pltpu.SemaphoreType.DMA,
            pltpu.SemaphoreType.DMA((5 + 2 * rounds,)),
            pltpu.SemaphoreType.DMA((2,)),
            pltpu.SemaphoreType.DMA((rounds,)),
            pltpu.SemaphoreType.DMA((rounds,)),
            pltpu.SemaphoreType.DMA((rounds,)),
            pltpu.SemaphoreType.DMA,
        ],
        compiler_params=pltpu.CompilerParams(
            collective_id=0, has_side_effects=True, vmem_limit_bytes=48 * 1024 * 1024
        ),
    )(*(pltpu.with_memory_space_constraint(x, pltpu.HBM) for x in inputs))
    dist, means = pl.pallas_call(
        finish,
        name="finish",
        out_shape=(
            jax.ShapeDtypeStruct(flat, jnp.float32),
            jax.ShapeDtypeStruct((1, rounds), jnp.float32),
        ),
        in_specs=[vmem],
        out_specs=(vmem, vmem),
        compiler_params=pltpu.CompilerParams(vmem_limit_bytes=1024 * 1024),
    )(both)
    return dist.reshape(rows), means.reshape(rounds, 1)


def solution(mesh):
    placed = (P(("grp", "dev"), None), P(("grp", "dev")), P())
    return jax.shard_map(
        body,
        mesh=mesh,
        in_specs=placed,
        out_specs=(P(("grp", "dev")), P(None, "grp")),
        check_vma=False,
    )
```

```python
import functools

import jax
import jax.numpy as jnp
from jax import lax
from jax.experimental import pallas as pl
from jax.experimental.pallas import tpu as pltpu
from jax.sharding import PartitionSpec as P

MESH = pl.DeviceIdType.MESH
PICK = 32
CHUNK = 256
LANES = 128
PIECE = 128
PIECES = 7
LAG = 4
EDGE = 8
NORM_ROWS = 16
NORM_PARTS = 2


def tile_of(emb, j):
    return emb[pl.ds(pl.multiple_of(j * CHUNK, CHUNK), CHUNK), :]


def row_norms(emb, norms, accs, part):
    width = emb.shape[1]
    ones = jnp.ones((NORM_ROWS, width), jnp.bfloat16)
    steps = 4

    trips = emb.shape[0] // CHUNK // (2 * steps)

    @pl.loop(part * trips // NORM_PARTS, (part + 1) * trips // NORM_PARTS)
    def _(t):
        for i in range(steps):
            for q in range(2):
                j = (t * steps + i) * 2 + q
                x = tile_of(emb, j).astype(jnp.float32)
                square = x * x
                high = square.astype(jnp.bfloat16)
                low = (square - high.astype(jnp.float32)).astype(jnp.bfloat16)
                acc = accs[q][PIECES + i]
                for part in (high, low):
                    pltpu.matmul_push_rhs(part, staging_register=0, mxu_index=q, transpose=True)
                    pltpu.matmul_acc_lhs(acc, ones, load_staged_rhs=0)
                total = pltpu.matmul_pop(acc)
                for k in range(CHUNK // LANES):
                    norms[pl.ds(j * (CHUNK // LANES) + k, 1), :] = total[
                        0:1, k * LANES : (k + 1) * LANES
                    ]


def push_tiles(emb, t):
    for q in range(2):
        pltpu.matmul_push_rhs(
            tile_of(emb, t * 2 + q), staging_register=0, mxu_index=q, transpose=True
        )


def half_norms(center, half, unit):
    chips, share, width = center.shape
    wide_c = center[...].reshape(chips * share, width).astype(jnp.float32)
    half[unit] = jnp.broadcast_to(
        0.5 * jnp.sum(wide_c * wide_c, axis=1, keepdims=True), (chips * share, LANES)
    )


def nearest_of(emb, sides, half, best, accs, between):
    chips, share, width = sides[0].shape
    trips = emb.shape[0] // CHUNK // 2
    pieces = chips * share // PIECE
    pending = []
    run = {}

    def pop():
        unit, t, p, use = pending.pop(0)
        offset = half[unit, pl.ds(p * PIECE, PIECE), :]
        for q in range(2):
            value = pltpu.matmul_pop(use[q])
            for k in range(CHUNK // LANES):
                short = value[:, k * LANES : (k + 1) * LANES] - offset
                short = jnp.max(short.reshape(PIECE // 8, 8, LANES), axis=0)
                run[q, k] = jnp.maximum(run[q, k], short) if p else short
        if p == pieces - 1:
            for (q, k), value in list(run.items()):
                row = (t * 2 + q) * (CHUNK // LANES) + k
                value = jnp.max(value, axis=0, keepdims=True)
                if unit:
                    value = jnp.maximum(value, best[pl.ds(row, 1), :])
                best[pl.ds(row, 1), :] = value

    count = 0
    for unit in range(2):
        if unit:
            between()
        half_norms(sides[unit], half, unit)
        for t in range(trips):
            for p in range(pieces):
                lhs = sides[unit][pl.ds(p * PIECE // share, PIECE // share)].reshape(PIECE, width)
                use = [accs[q][count % PIECES] for q in range(2)]
                count += 1
                for q in range(2):
                    pltpu.matmul_acc_lhs(use[q], lhs, load_staged_rhs=None if p else 0)
                if p == 0:
                    push_tiles(emb, (t + 1) % trips)
                pending.append((unit, t, p, use))
                if len(pending) > LAG:
                    pop()
    while pending:
        pop()


def kernel(sizes, *refs):
    specs = [
        pltpu.ACC(q)((rows, CHUNK), jnp.float32)
        for q in range(2)
        for rows in [PIECE] * PIECES + [NORM_ROWS] * 4
    ]

    def inner(*accs):
        half = len(accs) // 2
        run_kernel(sizes, *refs, (accs[:half], accs[half:]))

    pl.run_scoped(inner, *specs)


def arrived(ref, sem):
    pltpu.make_async_copy(ref, ref, sem).wait()


def run_kernel(
    sizes,
    ids_hbm,
    emb_hbm,
    prior_hbm,
    both_ref,
    ids,
    places,
    spots,
    emb,
    prior,
    wide,
    pick_wide,
    picks,
    pair,
    sums,
    parts,
    blocks,
    centers,
    half,
    norms,
    best,
    nearest,
    own_rows,
    own_total,
    totals,
    load_sem,
    id_sem,
    place_sem,
    prior_sem,
    send_sem,
    pair_sem,
    part_sem,
    block_sem,
    center_sem,
    relay_sem,
    total_sem,
    accs,
):
    groups, devs, rounds, seeds, rows, width = sizes
    me_grp = lax.axis_index("grp")
    me = lax.axis_index("dev")
    cores = 2
    chips = devs // cores
    chip, core = me // cores, lax.rem(me, cores)
    base = (me_grp * devs + me) * rows
    share = seeds // devs
    pieces = load_sem.shape[0]
    piece = rows // pieces
    tail = rounds - groups
    reach = (1, 3, 2)

    def load(k):
        return pltpu.make_async_copy(
            emb_hbm.at[pl.ds(k * piece, piece)], emb.at[pl.ds(k * piece, piece)], load_sem.at[k]
        )

    def load_ids(slot):
        which = me_grp + groups * slot
        return pltpu.make_async_copy(
            ids_hbm.at[pl.ds(which, 1)], ids.at[slot], id_sem.at[slot]
        )

    def place(slot):
        load_ids(slot).wait()
        places[slot] = 2 * jnp.clip(ids[slot] - base, -1, rows) + EDGE

    def move_places(slot):
        return pltpu.make_async_copy(places.at[slot], spots[slot], place_sem.at[slot])

    load_ids(0).start()
    for k in range(pieces):
        load(k).start()
    load_prior = pltpu.make_async_copy(prior_hbm, prior, prior_sem)
    load_prior.start()

    @pl.when(me_grp < tail)
    def _():
        load_ids(1).start()

    barrier = pltpu.get_barrier_semaphore()

    @pl.loop(1, devs)
    def _(p):
        pl.semaphore_signal(barrier, inc=1, device_id={"dev": lax.rem(me + p, devs)}, device_id_type=MESH)

    for p in range(1, groups):
        pl.semaphore_signal(
            barrier, inc=1, device_id={"grp": lax.rem(me_grp + p, groups)}, device_id_type=MESH
        )

    for edge in (0, EDGE + 2 * rows):
        wide[pl.ds(edge, EDGE), :] = jnp.zeros((EDGE, LANES), jnp.float32)
    for k in range(pieces):
        load(k).wait()
        if k == 1:
            place(0)

            @pl.when(me_grp < tail)
            def _():
                place(1)

        if k == pieces // 2:
            move_places(0).start()

            @pl.when(me_grp < tail)
            def _():
                move_places(1).start()

        @pl.loop(0, piece // 128)
        def _(t, k=k):
            at = pl.multiple_of(k * piece + t * 128, 128)
            x = emb[pl.ds(at, 128), :].astype(jnp.float32)
            for h in range(2):
                wide[pl.ds(EDGE + 2 * at + h, 128, stride=2), :] = x[:, h * LANES : (h + 1) * LANES]

    def pick(slot, side):
        each = PICK // share

        @pl.loop(0, chips // each)
        def _(t):
            for v in range(each):
                c = t * each + v
                to = c * cores + side
                row = pl.multiple_of(to * 2 * share, 2 * share)
                for u in range(share):
                    at = spots[slot][0, to * share + u]
                    pick_wide[pl.ds(row + 2 * u, 2), :] = wide[pl.ds(at, 2), :]
                for h in range(2):
                    picks[slot, side, c, :, h * LANES : (h + 1) * LANES] = pick_wide[
                        pl.ds(row + h, share, stride=2), :
                    ].astype(jnp.bfloat16)

    def pair_up(slot):
        pltpu.make_async_remote_copy(
            src_ref=picks.at[slot, 1 - core],
            dst_ref=pair.at[slot],
            send_sem=send_sem.at[5 + 2 * rounds + slot],
            recv_sem=pair_sem.at[slot],
            device_id={"dev": chip * cores + 1 - core},
            device_id_type=MESH,
        ).start()

    def scatter(slot):
        arrived(pair.at[slot], pair_sem.at[slot])

        def add(q):
            c = lax.rem(chip + 1 + q, chips)
            total = picks[slot, core, c].astype(jnp.float32) + pair[slot, c].astype(jnp.float32)
            sums[slot, c] = total.astype(jnp.bfloat16)

        def send(q):
            c = lax.rem(chip + 1 + q, chips)
            pltpu.make_async_remote_copy(
                src_ref=sums.at[slot, c],
                dst_ref=parts.at[slot, chip],
                send_sem=send_sem.at[slot],
                recv_sem=part_sem.at[slot],
                device_id={"dev": c * cores + core},
                device_id_type=MESH,
            ).start()

        add(0)

        @pl.loop(1, chips)
        def _(q):
            add(q)
            send(q - 1)

        parts[slot, chip] = sums[slot, chip]

    def take(slot):
        arrived(parts.at[slot, pl.ds(0, chips - 1)], part_sem.at[slot])
        total = jnp.sum(parts[slot].astype(jnp.float32), axis=0)
        blocks[me_grp + groups * slot] = total.astype(jnp.bfloat16)

    def trade(slot):
        index = me_grp + groups * slot
        for p in reach:
            pltpu.make_async_remote_copy(
                src_ref=blocks.at[index],
                dst_ref=blocks.at[index],
                send_sem=send_sem.at[2 + slot],
                recv_sem=block_sem.at[index],
                device_id={"grp": lax.rem(me_grp + p, groups)},
                device_id_type=MESH,
            ).start()

    def spread(r):
        @pl.loop(1, chips)
        def _(p):
            pltpu.make_async_remote_copy(
                src_ref=blocks.at[r],
                dst_ref=centers.at[r, core, chip],
                send_sem=send_sem.at[4 + r],
                recv_sem=center_sem.at[r],
                device_id={"dev": lax.rem(chip + p, chips) * cores + core},
                device_id_type=MESH,
            ).start()

        centers[r, core, chip] = blocks[r]

    def relay(r):
        arrived(centers.at[r, 0, pl.ds(0, chips - 1)], center_sem.at[r])
        pltpu.make_async_remote_copy(
            src_ref=centers.at[r, core],
            dst_ref=centers.at[r, core],
            send_sem=send_sem.at[4 + rounds + r],
            recv_sem=relay_sem.at[r],
            device_id={"dev": chip * cores + 1 - core},
            device_id_type=MESH,
        ).start()

    def turn(i):
        lap, j = i // groups, lax.rem(i, groups)
        ahead = j + j // 2 * (groups + 1 - 2 * j)
        return lap * groups + lax.rem(me_grp * (1 - lap) + ahead, groups)

    move_places(0).wait()
    pick(0, 1 - core)
    pl.semaphore_wait(barrier, devs - 1 + groups - 1)
    pair_up(0)

    @pl.when(me_grp < tail)
    def _():
        move_places(1).wait()
        pick(1, 1 - core)
        pair_up(1)

    pick(0, core)
    scatter(0)

    @pl.when(me_grp < tail)
    def _():
        pick(1, core)
        scatter(1)

    row_norms(emb, norms, accs, 0)
    take(0)
    trade(0)
    spread(me_grp)

    row_norms(emb, norms, accs, 1)
    for p in reach:
        near = lax.rem(me_grp + p, groups)
        arrived(blocks.at[near], block_sem.at[near])
        spread(near)

    @pl.when(me_grp < tail)
    def _():
        take(1)
        trade(1)

    push_tiles(emb, 0)

    @pl.loop(0, rounds)
    def _(i):
        r = turn(i)
        relay(r)

        @pl.when(i == 1)
        def _():
            for index in range(groups, rounds):

                @pl.when(me_grp != index - groups)
                def _():
                    arrived(blocks.at[index], block_sem.at[index])

                spread(index)

        def between():
            arrived(centers.at[r, 0], relay_sem.at[r])

        sides = (centers.at[r, core], centers.at[r, 1 - core])
        nearest_of(emb, sides, half, best, accs, between)
        nearest[r] = jnp.maximum(norms[...] - 2.0 * best[...], 0.0) / float(width)

    for q in range(2):
        unused = accs[q][PIECES]
        pltpu.matmul_acc_lhs(unused, jnp.zeros((NORM_ROWS, width), jnp.bfloat16), load_staged_rhs=0)
        pltpu.matmul_pop(unused)

    load_prior.wait()
    current = prior[...]
    own_rows[...] = jnp.zeros((8, LANES), jnp.float32)
    for r in range(rounds):
        current = jnp.minimum(current, nearest[r])
        own_rows[pl.ds(r, 1), :] = jnp.sum(current, axis=0, keepdims=True)
    both_ref[pl.ds(0, rows // LANES), :] = current
    sums = jnp.broadcast_to(jnp.sum(own_rows[...], axis=1, keepdims=True), (8, LANES))
    lane = lax.broadcasted_iota(jnp.int32, (8, LANES), 1)
    row = lax.broadcasted_iota(jnp.int32, (8, LANES), 0)
    own_total[...] = jnp.sum(jnp.where(lane == row, sums, 0.0), axis=0, keepdims=True)

    @pl.loop(1, devs)
    def _(p):
        pltpu.make_async_remote_copy(
            src_ref=own_total,
            dst_ref=totals.at[me],
            send_sem=send_sem.at[4 + 2 * rounds],
            recv_sem=total_sem,
            device_id={"dev": lax.rem(me + p, devs)},
            device_id_type=MESH,
        ).start()

    totals[pl.ds(me, 1)] = own_total[...][None]
    arrived(totals.at[pl.ds(0, devs - 1)], total_sem)
    mean = jnp.sum(totals[...], axis=0) / float(rows * devs)
    both_ref[pl.ds(rows // LANES, 8), :] = jnp.broadcast_to(mean, (8, LANES))

    arrived(parts.at[0, pl.ds(0, chips - 1)], send_sem.at[0])
    arrived(pair.at[0], send_sem.at[5 + 2 * rounds])
    arrived(blocks.at[pl.ds(0, groups - 1)], send_sem.at[2])

    @pl.when(me_grp < tail)
    def _():
        arrived(parts.at[1, pl.ds(0, chips - 1)], send_sem.at[1])
        arrived(pair.at[1], send_sem.at[6 + 2 * rounds])
        arrived(blocks.at[pl.ds(0, groups - 1)], send_sem.at[3])

    for r in range(rounds):
        arrived(centers.at[r, 0, pl.ds(0, chips - 1)], send_sem.at[4 + r])
        arrived(centers.at[r, 0], send_sem.at[4 + rounds + r])
    arrived(totals.at[pl.ds(0, devs - 1)], send_sem.at[4 + 2 * rounds])


def finish(both, dist_ref, mean_ref):
    count = dist_ref.shape[0]
    dist_ref[...] = both[pl.ds(0, count), :]
    mean_ref[...] = both[pl.ds(count, 1), : mean_ref.shape[1]]


def body(embeddings, prior_dist, seed_ids):
    rows, width = embeddings.shape
    rounds, seeds = seed_ids.shape
    groups, devs = lax.axis_size("grp"), lax.axis_size("dev")
    share = seeds // devs
    slots = -(-rounds // groups)
    sizes = (groups, devs, rounds, seeds, rows, width)
    flat = (rows // LANES, LANES)
    vmem = pl.BlockSpec(memory_space=pltpu.VMEM)
    hbm = pl.BlockSpec(memory_space=pltpu.HBM)
    inputs = (seed_ids, embeddings, prior_dist.reshape(flat))
    both = pl.pallas_call(
        functools.partial(kernel, sizes),
        name="seeding",
        out_shape=jax.ShapeDtypeStruct((rows // LANES + 8, LANES), jnp.float32),
        in_specs=[hbm, hbm, hbm],
        out_specs=vmem,
        scratch_shapes=[
            pltpu.VMEM((slots, 1, seeds), jnp.int32),
            pltpu.VMEM((slots, 1, seeds), jnp.int32),
            [pltpu.SMEM((1, seeds), jnp.int32)] * slots,
            pltpu.VMEM((rows, width), jnp.bfloat16),
            pltpu.VMEM(flat, jnp.float32),
            pltpu.VMEM((2 * rows + 2 * EDGE, LANES), jnp.float32),
            pltpu.VMEM((2 * seeds, LANES), jnp.float32),
            pltpu.VMEM((slots, 2, devs // 2, share, width), jnp.bfloat16),
            pltpu.VMEM((slots, devs // 2, share, width), jnp.bfloat16),
            pltpu.VMEM((slots, devs // 2, share, width), jnp.bfloat16),
            pltpu.VMEM((slots, devs // 2, share, width), jnp.bfloat16),
            pltpu.VMEM((rounds, share, width), jnp.bfloat16),
            pltpu.VMEM((rounds, 2, devs // 2, share, width), jnp.bfloat16),
            pltpu.VMEM((2, seeds // 2, LANES), jnp.float32),
            pltpu.VMEM(flat, jnp.float32),
            pltpu.VMEM(flat, jnp.float32),
            pltpu.VMEM((rounds, *flat), jnp.float32),
            pltpu.VMEM((8, LANES), jnp.float32),
            pltpu.VMEM((1, LANES), jnp.float32),
            pltpu.VMEM((devs, 1, LANES), jnp.float32),
            pltpu.SemaphoreType.DMA((8,)),
            pltpu.SemaphoreType.DMA((slots,)),
            pltpu.SemaphoreType.DMA((slots,)),
            pltpu.SemaphoreType.DMA,
            pltpu.SemaphoreType.DMA((7 + 2 * rounds,)),
            pltpu.SemaphoreType.DMA((2,)),
            pltpu.SemaphoreType.DMA((2,)),
            pltpu.SemaphoreType.DMA((rounds,)),
            pltpu.SemaphoreType.DMA((rounds,)),
            pltpu.SemaphoreType.DMA((rounds,)),
            pltpu.SemaphoreType.DMA,
        ],
        compiler_params=pltpu.CompilerParams(
            collective_id=0, has_side_effects=True, vmem_limit_bytes=48 * 1024 * 1024
        ),
    )(*(pltpu.with_memory_space_constraint(x, pltpu.HBM) for x in inputs))
    dist, means = pl.pallas_call(
        finish,
        name="finish",
        out_shape=(
            jax.ShapeDtypeStruct(flat, jnp.float32),
            jax.ShapeDtypeStruct((1, rounds), jnp.float32),
        ),
        in_specs=[vmem],
        out_specs=(vmem, vmem),
        compiler_params=pltpu.CompilerParams(vmem_limit_bytes=1024 * 1024),
    )(both)
    return dist.reshape(rows), means.reshape(rounds, 1)


def solution(mesh):
    placed = (P(("grp", "dev"), None), P(("grp", "dev")), P())
    return jax.shard_map(
        body,
        mesh=mesh,
        in_specs=placed,
        out_specs=(P(("grp", "dev")), P(None, "grp")),
        check_vma=False,
    )
```

```python
import functools
import math

import jax
import jax.numpy as jnp
from jax import lax
from jax.experimental import pallas as pl
from jax.experimental.pallas import tpu as pltpu
from jax.sharding import PartitionSpec as P

MESH = pl.DeviceIdType.MESH
PICK = 32
CHUNK = 256
LANES = 128
PIECE = 128
PIECES = 7
UNROLL = 3
LAG = 4
EDGE = 8
NORM_ROWS = 16
NORM_PARTS = 2


def tile_of(emb, j):
    return emb[pl.ds(pl.multiple_of(j * CHUNK, CHUNK), CHUNK), :]


def row_norms(emb, norms, accs, part):
    width = emb.shape[1]
    ones = jnp.ones((NORM_ROWS, width), jnp.bfloat16)
    steps = 4

    trips = emb.shape[0] // CHUNK // (2 * steps)

    @pl.loop(part * trips // NORM_PARTS, (part + 1) * trips // NORM_PARTS)
    def _(t):
        for i in range(steps):
            for q in range(2):
                j = (t * steps + i) * 2 + q
                x = tile_of(emb, j).astype(jnp.float32)
                square = x * x
                high = square.astype(jnp.bfloat16)
                low = (square - high.astype(jnp.float32)).astype(jnp.bfloat16)
                acc = accs[q][PIECES + i]
                for part in (high, low):
                    pltpu.matmul_push_rhs(part, staging_register=0, mxu_index=q, transpose=True)
                    pltpu.matmul_acc_lhs(acc, ones, load_staged_rhs=0)
                total = pltpu.matmul_pop(acc)
                for k in range(CHUNK // LANES):
                    norms[pl.ds(j * (CHUNK // LANES) + k, 1), :] = total[
                        0:1, k * LANES : (k + 1) * LANES
                    ]


def push_tiles(emb, t):
    for q in range(2):
        pltpu.matmul_push_rhs(
            tile_of(emb, t * 2 + q), staging_register=0, mxu_index=q, transpose=True
        )


def half_norms(center, half, unit):
    chips, share, width = center.shape
    wide_c = center[...].reshape(chips * share, width).astype(jnp.float32)
    half[unit] = jnp.broadcast_to(
        0.5 * jnp.sum(wide_c * wide_c, axis=1, keepdims=True), (chips * share, LANES)
    )


class Stream:
    def __init__(self, emb, half, accs):
        self.emb, self.half, self.accs = emb, half, accs
        self.pending = []
        self.run = {}
        self.count = 0
        self.units = 0

    def pop(self):
        unit, side, best, t, p, pieces, use = self.pending.pop(0)
        offset = self.half[unit, pl.ds(p * PIECE, PIECE), :]
        for q in range(2):
            value = pltpu.matmul_pop(use[q])
            for k in range(CHUNK // LANES):
                short = value[:, k * LANES : (k + 1) * LANES] - offset
                short = jnp.max(short.reshape(PIECE // 8, 8, LANES), axis=0)
                self.run[q, k] = jnp.maximum(self.run[q, k], short) if p else short
        if p == pieces - 1:
            for (q, k), value in list(self.run.items()):
                row = (t * 2 + q) * (CHUNK // LANES) + k
                value = jnp.max(value, axis=0, keepdims=True)
                if side:
                    value = jnp.maximum(value, best[pl.ds(row, 1), :])
                best[pl.ds(row, 1), :] = value

    def side(self, center, side, best):
        chips, share, width = center.shape
        trips = self.emb.shape[0] // CHUNK // 2
        pieces = chips * share // PIECE
        half_norms(center, self.half, self.units)
        for t in range(trips):
            for p in range(pieces):
                lhs = center[pl.ds(p * PIECE // share, PIECE // share)].reshape(PIECE, width)
                use = [self.accs[q][self.count % PIECES] for q in range(2)]
                self.count += 1
                for q in range(2):
                    pltpu.matmul_acc_lhs(use[q], lhs, load_staged_rhs=None if p else 0)
                if p == 0:
                    push_tiles(self.emb, (t + 1) % trips)
                self.pending.append((self.units, side, best, t, p, pieces, use))
                if len(self.pending) > LAG:
                    self.pop()
        self.units += 1

    def finish(self):
        while self.pending:
            self.pop()


def kernel(sizes, *refs):
    specs = [
        pltpu.ACC(q)((rows, CHUNK), jnp.float32)
        for q in range(2)
        for rows in [PIECE] * PIECES + [NORM_ROWS] * 4
    ]

    def inner(*accs):
        half = len(accs) // 2
        run_kernel(sizes, *refs, (accs[:half], accs[half:]))

    pl.run_scoped(inner, *specs)


def far_first(side):
    ring = lambda d: min(d, side - d)
    steps = [(a, b) for a in range(side) for b in range(side) if (a, b) != (0, 0)]
    return sorted(steps, key=lambda s: -ring(s[0]) - ring(s[1]))


def arrived(ref, sem):
    pltpu.make_async_copy(ref, ref, sem).wait()


def run_kernel(
    sizes,
    ids_hbm,
    emb_hbm,
    prior_hbm,
    both_ref,
    ids,
    places,
    spots,
    emb,
    prior,
    wide,
    pick_wide,
    picks,
    pair,
    sums,
    parts,
    blocks,
    centers,
    half,
    norms,
    nearest,
    own_rows,
    own_total,
    totals,
    load_sem,
    id_sem,
    place_sem,
    prior_sem,
    send_sem,
    pair_sem,
    part_sem,
    block_sem,
    center_sem,
    relay_sem,
    total_sem,
    accs,
):
    groups, devs, rounds, seeds, rows, width = sizes
    me_grp = lax.axis_index("grp")
    me = lax.axis_index("dev")
    cores = 2
    chips = devs // cores
    chip, core = me // cores, lax.rem(me, cores)
    base = (me_grp * devs + me) * rows
    side = math.isqrt(chips)
    share = seeds // devs
    pieces = load_sem.shape[0]
    piece = rows // pieces
    tail = rounds - groups
    reach = (1, 3, 2)

    def chip_at(step):
        a, b = step
        return lax.rem(chip // side + a, side) * side + lax.rem(chip + b, side)

    def load(k):
        return pltpu.make_async_copy(
            emb_hbm.at[pl.ds(k * piece, piece)], emb.at[pl.ds(k * piece, piece)], load_sem.at[k]
        )

    def load_ids(slot):
        which = me_grp + groups * slot
        return pltpu.make_async_copy(
            ids_hbm.at[pl.ds(which, 1)], ids.at[slot], id_sem.at[slot]
        )

    def place(slot):
        load_ids(slot).wait()
        places[slot] = 2 * jnp.clip(ids[slot] - base, -1, rows) + EDGE

    def move_places(slot):
        return pltpu.make_async_copy(places.at[slot], spots[slot], place_sem.at[slot])

    load_ids(0).start()

    @pl.when(me_grp < tail)
    def _():
        load_ids(1).start()

    for k in range(pieces):
        load(k).start()
    load_prior = pltpu.make_async_copy(prior_hbm, prior, prior_sem)
    load_prior.start()

    barrier = pltpu.get_barrier_semaphore()

    @pl.loop(1, devs)
    def _(p):
        pl.semaphore_signal(barrier, inc=1, device_id={"dev": lax.rem(me + p, devs)}, device_id_type=MESH)

    for p in range(1, groups):
        pl.semaphore_signal(
            barrier, inc=1, device_id={"grp": lax.rem(me_grp + p, groups)}, device_id_type=MESH
        )

    for edge in (0, EDGE + 2 * rows):
        wide[pl.ds(edge, EDGE), :] = jnp.zeros((EDGE, LANES), jnp.float32)
    for k in range(pieces):
        load(k).wait()
        if k == 1:
            place(0)

            @pl.when(me_grp < tail)
            def _():
                place(1)

        if k == pieces // 2:
            move_places(0).start()

            @pl.when(me_grp < tail)
            def _():
                move_places(1).start()

        @pl.loop(0, piece // 128)
        def _(t, k=k):
            at = pl.multiple_of(k * piece + t * 128, 128)
            x = emb[pl.ds(at, 128), :].astype(jnp.float32)
            for h in range(2):
                wide[pl.ds(EDGE + 2 * at + h, 128, stride=2), :] = x[:, h * LANES : (h + 1) * LANES]

    def pick(slot, side):
        each = PICK // share

        @pl.loop(0, chips // each)
        def _(t):
            for v in range(each):
                c = t * each + v
                to = c * cores + side
                row = pl.multiple_of(to * 2 * share, 2 * share)
                for u in range(share):
                    at = spots[slot][0, to * share + u]
                    pick_wide[pl.ds(row + 2 * u, 2), :] = wide[pl.ds(at, 2), :]
                for h in range(2):
                    picks[slot, side, c, :, h * LANES : (h + 1) * LANES] = pick_wide[
                        pl.ds(row + h, share, stride=2), :
                    ].astype(jnp.bfloat16)

    def pair_up(slot):
        pltpu.make_async_remote_copy(
            src_ref=picks.at[slot, 1 - core],
            dst_ref=pair.at[slot],
            send_sem=send_sem.at[5 + 2 * rounds + slot],
            recv_sem=pair_sem.at[slot],
            device_id={"dev": chip * cores + 1 - core},
            device_id_type=MESH,
        ).start()

    def scatter(slot):
        arrived(pair.at[slot], pair_sem.at[slot])

        def add(c):
            total = picks[slot, core, c].astype(jnp.float32) + pair[slot, c].astype(jnp.float32)
            sums[slot, c] = total.astype(jnp.bfloat16)

        def send(c):
            pltpu.make_async_remote_copy(
                src_ref=sums.at[slot, c],
                dst_ref=parts.at[slot, chip],
                send_sem=send_sem.at[slot],
                recv_sem=part_sem.at[slot],
                device_id={"dev": c * cores + core},
                device_id_type=MESH,
            ).start()

        order = [chip_at(step) for step in far_first(side)]
        add(order[0])
        for q in range(1, chips - 1):
            add(order[q])
            send(order[q - 1])
        add(chip)
        send(order[-1])
        parts[slot, chip] = sums[slot, chip]

    def take(slot):
        arrived(parts.at[slot, pl.ds(0, chips - 1)], part_sem.at[slot])
        total = jnp.sum(parts[slot].astype(jnp.float32), axis=0)
        blocks[me_grp + groups * slot] = total.astype(jnp.bfloat16)

    def trade(slot):
        index = me_grp + groups * slot
        for p in reach:
            pltpu.make_async_remote_copy(
                src_ref=blocks.at[index],
                dst_ref=blocks.at[index],
                send_sem=send_sem.at[2 + slot],
                recv_sem=block_sem.at[index],
                device_id={"grp": lax.rem(me_grp + p, groups)},
                device_id_type=MESH,
            ).start()

    def spread(r):
        for step in far_first(side):
            pltpu.make_async_remote_copy(
                src_ref=blocks.at[r],
                dst_ref=centers.at[r, core, chip],
                send_sem=send_sem.at[4 + r],
                recv_sem=center_sem.at[r],
                device_id={"dev": chip_at(step) * cores + core},
                device_id_type=MESH,
            ).start()

        centers[r, core, chip] = blocks[r]

    def relay(r):
        arrived(centers.at[r, 0, pl.ds(0, chips - 1)], center_sem.at[r])
        pltpu.make_async_remote_copy(
            src_ref=centers.at[r, core],
            dst_ref=centers.at[r, core],
            send_sem=send_sem.at[4 + rounds + r],
            recv_sem=relay_sem.at[r],
            device_id={"dev": chip * cores + 1 - core},
            device_id_type=MESH,
        ).start()

    def turn(i):
        lap, j = i // groups, lax.rem(i, groups)
        ahead = j + j // 2 * (groups + 1 - 2 * j)
        return lap * groups + lax.rem(me_grp * (1 - lap) + ahead, groups)

    move_places(0).wait()
    pick(0, 1 - core)
    pl.semaphore_wait(barrier, devs - 1 + groups - 1)
    pair_up(0)

    @pl.when(me_grp < tail)
    def _():
        move_places(1).wait()
        pick(1, 1 - core)
        pair_up(1)

    pick(0, core)
    scatter(0)

    @pl.when(me_grp < tail)
    def _():
        pick(1, core)
        scatter(1)

    row_norms(emb, norms, accs, 0)
    take(0)
    trade(0)
    spread(me_grp)

    row_norms(emb, norms, accs, 1)
    for p in reach:
        near = lax.rem(me_grp + p, groups)
        arrived(blocks.at[near], block_sem.at[near])
        spread(near)

    @pl.when(me_grp < tail)
    def _():
        take(1)
        trade(1)

    push_tiles(emb, 0)

    @pl.loop(0, rounds // UNROLL)
    def _(step):
        stream = Stream(emb, half, accs)
        for k in range(UNROLL):
            i = step * UNROLL + k
            r = turn(i)
            relay(r)

            @pl.when(i == 1)
            def _():
                for index in range(groups, rounds):

                    @pl.when(me_grp != index - groups)
                    def _():
                        arrived(blocks.at[index], block_sem.at[index])

                    spread(index)

            stream.side(centers.at[r, core], 0, nearest.at[r])
            arrived(centers.at[r, 0], relay_sem.at[r])
            stream.side(centers.at[r, 1 - core], 1, nearest.at[r])
        stream.finish()

    for q in range(2):
        unused = accs[q][PIECES]
        pltpu.matmul_acc_lhs(unused, jnp.zeros((NORM_ROWS, width), jnp.bfloat16), load_staged_rhs=0)
        pltpu.matmul_pop(unused)

    load_prior.wait()
    current = prior[...]
    own_rows[...] = jnp.zeros((8, LANES), jnp.float32)
    for r in range(rounds):
        gaps = jnp.maximum(norms[...] - 2.0 * nearest[r], 0.0) / float(width)
        current = jnp.minimum(current, gaps)
        own_rows[pl.ds(r, 1), :] = jnp.sum(current, axis=0, keepdims=True)
    both_ref[pl.ds(0, rows // LANES), :] = current
    sums = jnp.broadcast_to(jnp.sum(own_rows[...], axis=1, keepdims=True), (8, LANES))
    lane = lax.broadcasted_iota(jnp.int32, (8, LANES), 1)
    row = lax.broadcasted_iota(jnp.int32, (8, LANES), 0)
    own_total[...] = jnp.sum(jnp.where(lane == row, sums, 0.0), axis=0, keepdims=True)

    peers = [chip_at(step) * cores + c for step in far_first(side) for c in range(cores)]
    for peer in [*peers, chip * cores + 1 - core]:
        pltpu.make_async_remote_copy(
            src_ref=own_total,
            dst_ref=totals.at[me],
            send_sem=send_sem.at[4 + 2 * rounds],
            recv_sem=total_sem,
            device_id={"dev": peer},
            device_id_type=MESH,
        ).start()

    totals[pl.ds(me, 1)] = own_total[...][None]
    arrived(totals.at[pl.ds(0, devs - 1)], total_sem)
    mean = jnp.sum(totals[...], axis=0) / float(rows * devs)
    both_ref[pl.ds(rows // LANES, 8), :] = jnp.broadcast_to(mean, (8, LANES))

    arrived(parts.at[0, pl.ds(0, chips - 1)], send_sem.at[0])
    arrived(pair.at[0], send_sem.at[5 + 2 * rounds])
    arrived(blocks.at[pl.ds(0, groups - 1)], send_sem.at[2])

    @pl.when(me_grp < tail)
    def _():
        arrived(parts.at[1, pl.ds(0, chips - 1)], send_sem.at[1])
        arrived(pair.at[1], send_sem.at[6 + 2 * rounds])
        arrived(blocks.at[pl.ds(0, groups - 1)], send_sem.at[3])

    for r in range(rounds):
        arrived(centers.at[r, 0, pl.ds(0, chips - 1)], send_sem.at[4 + r])
        arrived(centers.at[r, 0], send_sem.at[4 + rounds + r])
    arrived(totals.at[pl.ds(0, devs - 1)], send_sem.at[4 + 2 * rounds])


def finish(both, dist_ref, mean_ref):
    count = dist_ref.shape[0]
    dist_ref[...] = both[pl.ds(0, count), :]
    mean_ref[...] = both[pl.ds(count, 1), : mean_ref.shape[1]]


def body(embeddings, prior_dist, seed_ids):
    rows, width = embeddings.shape
    rounds, seeds = seed_ids.shape
    groups, devs = lax.axis_size("grp"), lax.axis_size("dev")
    share = seeds // devs
    slots = -(-rounds // groups)
    sizes = (groups, devs, rounds, seeds, rows, width)
    flat = (rows // LANES, LANES)
    vmem = pl.BlockSpec(memory_space=pltpu.VMEM)
    hbm = pl.BlockSpec(memory_space=pltpu.HBM)
    inputs = (seed_ids, embeddings, prior_dist.reshape(flat))
    both = pl.pallas_call(
        functools.partial(kernel, sizes),
        name="seeding",
        out_shape=jax.ShapeDtypeStruct((rows // LANES + 8, LANES), jnp.float32),
        in_specs=[hbm, hbm, hbm],
        out_specs=vmem,
        scratch_shapes=[
            pltpu.VMEM((slots, 1, seeds), jnp.int32),
            pltpu.VMEM((slots, 1, seeds), jnp.int32),
            [pltpu.SMEM((1, seeds), jnp.int32)] * slots,
            pltpu.VMEM((rows, width), jnp.bfloat16),
            pltpu.VMEM(flat, jnp.float32),
            pltpu.VMEM((2 * rows + 2 * EDGE, LANES), jnp.float32),
            pltpu.VMEM((2 * seeds, LANES), jnp.float32),
            pltpu.VMEM((slots, 2, devs // 2, share, width), jnp.bfloat16),
            pltpu.VMEM((slots, devs // 2, share, width), jnp.bfloat16),
            pltpu.VMEM((slots, devs // 2, share, width), jnp.bfloat16),
            pltpu.VMEM((slots, devs // 2, share, width), jnp.bfloat16),
            pltpu.VMEM((rounds, share, width), jnp.bfloat16),
            pltpu.VMEM((rounds, 2, devs // 2, share, width), jnp.bfloat16),
            pltpu.VMEM((2 * UNROLL, seeds // 2, LANES), jnp.float32),
            pltpu.VMEM(flat, jnp.float32),
            pltpu.VMEM((rounds, *flat), jnp.float32),
            pltpu.VMEM((8, LANES), jnp.float32),
            pltpu.VMEM((1, LANES), jnp.float32),
            pltpu.VMEM((devs, 1, LANES), jnp.float32),
            pltpu.SemaphoreType.DMA((8,)),
            pltpu.SemaphoreType.DMA((slots,)),
            pltpu.SemaphoreType.DMA((slots,)),
            pltpu.SemaphoreType.DMA,
            pltpu.SemaphoreType.DMA((7 + 2 * rounds,)),
            pltpu.SemaphoreType.DMA((2,)),
            pltpu.SemaphoreType.DMA((2,)),
            pltpu.SemaphoreType.DMA((rounds,)),
            pltpu.SemaphoreType.DMA((rounds,)),
            pltpu.SemaphoreType.DMA((rounds,)),
            pltpu.SemaphoreType.DMA,
        ],
        compiler_params=pltpu.CompilerParams(
            collective_id=0, has_side_effects=True, vmem_limit_bytes=48 * 1024 * 1024
        ),
    )(*(pltpu.with_memory_space_constraint(x, pltpu.HBM) for x in inputs))
    dist, means = pl.pallas_call(
        finish,
        name="finish",
        out_shape=(
            jax.ShapeDtypeStruct(flat, jnp.float32),
            jax.ShapeDtypeStruct((1, rounds), jnp.float32),
        ),
        in_specs=[vmem],
        out_specs=(vmem, vmem),
        compiler_params=pltpu.CompilerParams(vmem_limit_bytes=1024 * 1024),
    )(both)
    return dist.reshape(rows), means.reshape(rounds, 1)


def solution(mesh):
    placed = (P(("grp", "dev"), None), P(("grp", "dev")), P())
    return jax.shard_map(
        body,
        mesh=mesh,
        in_specs=placed,
        out_specs=(P(("grp", "dev")), P(None, "grp")),
        check_vma=False,
    )
```

```python
import functools
import math

import jax
import jax.numpy as jnp
from jax import lax
from jax.experimental import pallas as pl
from jax.experimental.pallas import tpu as pltpu
from jax.sharding import PartitionSpec as P

MESH = pl.DeviceIdType.MESH
PICK = 32
CHUNK = 256
LANES = 128
PIECE = 128
PIECES = 7
UNROLL = 6
LAG = 4
EDGE = 8
NORM_ROWS = 16
NORM_PARTS = 2


def tile_of(emb, j):
    return emb[pl.ds(pl.multiple_of(j * CHUNK, CHUNK), CHUNK), :]


def row_norms(emb, norms, accs, part):
    width = emb.shape[1]
    ones = jnp.ones((NORM_ROWS, width), jnp.bfloat16)
    steps = 4

    trips = emb.shape[0] // CHUNK // (2 * steps)

    @pl.loop(part * trips // NORM_PARTS, (part + 1) * trips // NORM_PARTS)
    def _(t):
        for i in range(steps):
            for q in range(2):
                j = (t * steps + i) * 2 + q
                x = tile_of(emb, j).astype(jnp.float32)
                square = x * x
                high = square.astype(jnp.bfloat16)
                low = (square - high.astype(jnp.float32)).astype(jnp.bfloat16)
                acc = accs[q][PIECES + i]
                for part in (high, low):
                    pltpu.matmul_push_rhs(part, staging_register=0, mxu_index=q, transpose=True)
                    pltpu.matmul_acc_lhs(acc, ones, load_staged_rhs=0)
                total = pltpu.matmul_pop(acc)
                for k in range(CHUNK // LANES):
                    norms[pl.ds(j * (CHUNK // LANES) + k, 1), :] = total[
                        0:1, k * LANES : (k + 1) * LANES
                    ]


def push_tiles(emb, t):
    for q in range(2):
        pltpu.matmul_push_rhs(
            tile_of(emb, t * 2 + q), staging_register=0, mxu_index=q, transpose=True
        )


def half_norms(center, half, unit):
    chips, share, width = center.shape
    wide_c = center[...].reshape(chips * share, width).astype(jnp.float32)
    half[unit] = jnp.broadcast_to(
        0.5 * jnp.sum(wide_c * wide_c, axis=1, keepdims=True), (chips * share, LANES)
    )


class Stream:
    def __init__(self, emb, half, accs):
        self.emb, self.half, self.accs = emb, half, accs
        self.pending = []
        self.run = {}
        self.count = 0
        self.units = 0

    def pop(self):
        unit, side, best, t, p, pieces, use = self.pending.pop(0)
        offset = self.half[unit, pl.ds(p * PIECE, PIECE), :]
        for q in range(2):
            value = pltpu.matmul_pop(use[q])
            for k in range(CHUNK // LANES):
                short = value[:, k * LANES : (k + 1) * LANES] - offset
                short = jnp.max(short.reshape(PIECE // 8, 8, LANES), axis=0)
                self.run[q, k] = jnp.maximum(self.run[q, k], short) if p else short
        if p == pieces - 1:
            for (q, k), value in list(self.run.items()):
                row = (t * 2 + q) * (CHUNK // LANES) + k
                value = jnp.max(value, axis=0, keepdims=True)
                if side:
                    value = jnp.maximum(value, best[pl.ds(row, 1), :])
                best[pl.ds(row, 1), :] = value

    def side(self, center, side, best):
        chips, share, width = center.shape
        trips = self.emb.shape[0] // CHUNK // 2
        pieces = chips * share // PIECE
        half_norms(center, self.half, self.units)
        for t in range(trips):
            for p in range(pieces):
                lhs = center[pl.ds(p * PIECE // share, PIECE // share)].reshape(PIECE, width)
                use = [self.accs[q][self.count % PIECES] for q in range(2)]
                self.count += 1
                for q in range(2):
                    pltpu.matmul_acc_lhs(use[q], lhs, load_staged_rhs=None if p else 0)
                if p == 0:
                    push_tiles(self.emb, (t + 1) % trips)
                self.pending.append((self.units, side, best, t, p, pieces, use))
                if len(self.pending) > LAG:
                    self.pop()
        self.units += 1

    def finish(self):
        while self.pending:
            self.pop()


def kernel(sizes, *refs):
    specs = [
        pltpu.ACC(q)((rows, CHUNK), jnp.float32)
        for q in range(2)
        for rows in [PIECE] * PIECES + [NORM_ROWS] * 4
    ]

    def inner(*accs):
        half = len(accs) // 2
        run_kernel(sizes, *refs, (accs[:half], accs[half:]))

    pl.run_scoped(inner, *specs)


def far_first(side):
    ring = lambda d: min(d, side - d)
    steps = [(a, b) for a in range(side) for b in range(side) if (a, b) != (0, 0)]
    return sorted(steps, key=lambda s: -ring(s[0]) - ring(s[1]))


def arrived(ref, sem):
    pltpu.make_async_copy(ref, ref, sem).wait()


def run_kernel(
    sizes,
    ids_hbm,
    emb_hbm,
    prior_hbm,
    both_ref,
    ids,
    places,
    spots,
    emb,
    prior,
    wide,
    pick_wide,
    picks,
    pair,
    sums,
    parts,
    blocks,
    centers,
    half,
    norms,
    nearest,
    own_rows,
    own_total,
    totals,
    load_sem,
    id_sem,
    place_sem,
    prior_sem,
    send_sem,
    pair_sem,
    part_sem,
    block_sem,
    center_sem,
    relay_sem,
    total_sem,
    accs,
):
    groups, devs, rounds, seeds, rows, width = sizes
    me_grp = lax.axis_index("grp")
    me = lax.axis_index("dev")
    cores = 2
    chips = devs // cores
    chip, core = me // cores, lax.rem(me, cores)
    base = (me_grp * devs + me) * rows
    side = math.isqrt(chips)
    share = seeds // devs
    pieces = load_sem.shape[0]
    piece = rows // pieces
    tail = rounds - groups
    reach = (1, 3, 2)

    def chip_at(step):
        a, b = step
        return lax.rem(chip // side + a, side) * side + lax.rem(chip + b, side)

    def load(k):
        return pltpu.make_async_copy(
            emb_hbm.at[pl.ds(k * piece, piece)], emb.at[pl.ds(k * piece, piece)], load_sem.at[k]
        )

    def load_ids(slot):
        which = me_grp + groups * slot
        return pltpu.make_async_copy(
            ids_hbm.at[pl.ds(which, 1)], ids.at[slot], id_sem.at[slot]
        )

    def place(slot):
        load_ids(slot).wait()
        places[slot] = 2 * jnp.clip(ids[slot] - base, -1, rows) + EDGE

    def move_places(slot):
        return pltpu.make_async_copy(places.at[slot], spots[slot], place_sem.at[slot])

    load_ids(0).start()

    @pl.when(me_grp < tail)
    def _():
        load_ids(1).start()

    for k in range(pieces):
        load(k).start()
    load_prior = pltpu.make_async_copy(prior_hbm, prior, prior_sem)
    load_prior.start()

    barrier = pltpu.get_barrier_semaphore()

    peers = [chip_at(step) * cores + c for step in far_first(side) for c in range(cores)]
    peers.append(chip * cores + 1 - core)
    for peer in peers:
        pl.semaphore_signal(barrier, inc=1, device_id={"dev": peer}, device_id_type=MESH)

    for p in range(1, groups):
        pl.semaphore_signal(
            barrier, inc=1, device_id={"grp": lax.rem(me_grp + p, groups)}, device_id_type=MESH
        )

    for edge in (0, EDGE + 2 * rows):
        wide[pl.ds(edge, EDGE), :] = jnp.zeros((EDGE, LANES), jnp.float32)
    for k in range(pieces):
        load(k).wait()
        if k == 1:
            place(0)

            @pl.when(me_grp < tail)
            def _():
                place(1)

        if k == pieces // 2:
            move_places(0).start()

            @pl.when(me_grp < tail)
            def _():
                move_places(1).start()

        @pl.loop(0, piece // 128)
        def _(t, k=k):
            at = pl.multiple_of(k * piece + t * 128, 128)
            x = emb[pl.ds(at, 128), :].astype(jnp.float32)
            for h in range(2):
                wide[pl.ds(EDGE + 2 * at + h, 128, stride=2), :] = x[:, h * LANES : (h + 1) * LANES]

    def pick(slot, side):
        each = PICK // share

        @pl.loop(0, chips // each)
        def _(t):
            for v in range(each):
                c = t * each + v
                to = c * cores + side
                row = pl.multiple_of(to * 2 * share, 2 * share)
                for u in range(share):
                    at = spots[slot][0, to * share + u]
                    pick_wide[pl.ds(row + 2 * u, 2), :] = wide[pl.ds(at, 2), :]
                for h in range(2):
                    picks[slot, side, c, :, h * LANES : (h + 1) * LANES] = pick_wide[
                        pl.ds(row + h, share, stride=2), :
                    ].astype(jnp.bfloat16)

    def pair_up(slot):
        pltpu.make_async_remote_copy(
            src_ref=picks.at[slot, 1 - core],
            dst_ref=pair.at[slot],
            send_sem=send_sem.at[5 + 2 * rounds + slot],
            recv_sem=pair_sem.at[slot],
            device_id={"dev": chip * cores + 1 - core},
            device_id_type=MESH,
        ).start()

    def scatter(slot):
        arrived(pair.at[slot], pair_sem.at[slot])

        def add(c):
            total = picks[slot, core, c].astype(jnp.float32) + pair[slot, c].astype(jnp.float32)
            sums[slot, c] = total.astype(jnp.bfloat16)

        def send(c):
            pltpu.make_async_remote_copy(
                src_ref=sums.at[slot, c],
                dst_ref=parts.at[slot, chip],
                send_sem=send_sem.at[slot],
                recv_sem=part_sem.at[slot],
                device_id={"dev": c * cores + core},
                device_id_type=MESH,
            ).start()

        order = [chip_at(step) for step in far_first(side)]
        add(order[0])
        for q in range(1, chips - 1):
            add(order[q])
            send(order[q - 1])
        add(chip)
        send(order[-1])
        parts[slot, chip] = sums[slot, chip]

    def take(slot):
        arrived(parts.at[slot, pl.ds(0, chips - 1)], part_sem.at[slot])
        total = jnp.sum(parts[slot].astype(jnp.float32), axis=0)
        blocks[me_grp + groups * slot] = total.astype(jnp.bfloat16)

    def trade(slot):
        index = me_grp + groups * slot
        for p in reach:
            pltpu.make_async_remote_copy(
                src_ref=blocks.at[index],
                dst_ref=blocks.at[index],
                send_sem=send_sem.at[2 + slot],
                recv_sem=block_sem.at[index],
                device_id={"grp": lax.rem(me_grp + p, groups)},
                device_id_type=MESH,
            ).start()

    def spread(r):
        for step in far_first(side):
            pltpu.make_async_remote_copy(
                src_ref=blocks.at[r],
                dst_ref=centers.at[r, core, chip],
                send_sem=send_sem.at[4 + r],
                recv_sem=center_sem.at[r],
                device_id={"dev": chip_at(step) * cores + core},
                device_id_type=MESH,
            ).start()

        centers[r, core, chip] = blocks[r]

    def relay(r):
        arrived(centers.at[r, 0, pl.ds(0, chips - 1)], center_sem.at[r])
        pltpu.make_async_remote_copy(
            src_ref=centers.at[r, core],
            dst_ref=centers.at[r, core],
            send_sem=send_sem.at[4 + rounds + r],
            recv_sem=relay_sem.at[r],
            device_id={"dev": chip * cores + 1 - core},
            device_id_type=MESH,
        ).start()

    def turn(i):
        lap, j = i // groups, lax.rem(i, groups)
        ahead = j + j // 2 * (groups + 1 - 2 * j)
        return lap * groups + lax.rem(me_grp * (1 - lap) + ahead, groups)

    move_places(0).wait()
    pick(0, 1 - core)
    pl.semaphore_wait(barrier, devs - 1 + groups - 1)
    pair_up(0)

    @pl.when(me_grp < tail)
    def _():
        move_places(1).wait()
        pick(1, 1 - core)
        pair_up(1)

    pick(0, core)
    scatter(0)

    @pl.when(me_grp < tail)
    def _():
        pick(1, core)
        scatter(1)

    row_norms(emb, norms, accs, 0)
    take(0)
    trade(0)
    spread(me_grp)

    row_norms(emb, norms, accs, 1)
    for p in reach:
        near = lax.rem(me_grp + p, groups)
        arrived(blocks.at[near], block_sem.at[near])
        spread(near)

    @pl.when(me_grp < tail)
    def _():
        take(1)
        trade(1)

    push_tiles(emb, 0)

    @pl.loop(0, rounds // UNROLL)
    def _(step):
        stream = Stream(emb, half, accs)
        for k in range(UNROLL):
            i = step * UNROLL + k
            r = turn(i)
            relay(r)

            @pl.when(i == 1)
            def _():
                for index in range(groups, rounds):

                    @pl.when(me_grp != index - groups)
                    def _():
                        arrived(blocks.at[index], block_sem.at[index])

                    spread(index)

            stream.side(centers.at[r, core], 0, nearest.at[r])
            arrived(centers.at[r, 0], relay_sem.at[r])
            stream.side(centers.at[r, 1 - core], 1, nearest.at[r])
        stream.finish()

    for q in range(2):
        unused = accs[q][PIECES]
        pltpu.matmul_acc_lhs(unused, jnp.zeros((NORM_ROWS, width), jnp.bfloat16), load_staged_rhs=0)
        pltpu.matmul_pop(unused)

    load_prior.wait()
    current = prior[...]
    own_rows[...] = jnp.zeros((8, LANES), jnp.float32)
    for r in range(rounds):
        gaps = jnp.maximum(norms[...] - 2.0 * nearest[r], 0.0) / float(width)
        current = jnp.minimum(current, gaps)
        own_rows[pl.ds(r, 1), :] = jnp.sum(current, axis=0, keepdims=True)
    both_ref[pl.ds(0, rows // LANES), :] = current
    sums = jnp.broadcast_to(jnp.sum(own_rows[...], axis=1, keepdims=True), (8, LANES))
    lane = lax.broadcasted_iota(jnp.int32, (8, LANES), 1)
    row = lax.broadcasted_iota(jnp.int32, (8, LANES), 0)
    own_total[...] = jnp.sum(jnp.where(lane == row, sums, 0.0), axis=0, keepdims=True)

    for peer in peers:
        pltpu.make_async_remote_copy(
            src_ref=own_total,
            dst_ref=totals.at[me],
            send_sem=send_sem.at[4 + 2 * rounds],
            recv_sem=total_sem,
            device_id={"dev": peer},
            device_id_type=MESH,
        ).start()

    totals[pl.ds(me, 1)] = own_total[...][None]
    arrived(totals.at[pl.ds(0, devs - 1)], total_sem)
    mean = jnp.sum(totals[...], axis=0) / float(rows * devs)
    both_ref[pl.ds(rows // LANES, 8), :] = jnp.broadcast_to(mean, (8, LANES))

    arrived(parts.at[0, pl.ds(0, chips - 1)], send_sem.at[0])
    arrived(pair.at[0], send_sem.at[5 + 2 * rounds])
    arrived(blocks.at[pl.ds(0, groups - 1)], send_sem.at[2])

    @pl.when(me_grp < tail)
    def _():
        arrived(parts.at[1, pl.ds(0, chips - 1)], send_sem.at[1])
        arrived(pair.at[1], send_sem.at[6 + 2 * rounds])
        arrived(blocks.at[pl.ds(0, groups - 1)], send_sem.at[3])

    for r in range(rounds):
        arrived(centers.at[r, 0, pl.ds(0, chips - 1)], send_sem.at[4 + r])
        arrived(centers.at[r, 0], send_sem.at[4 + rounds + r])
    arrived(totals.at[pl.ds(0, devs - 1)], send_sem.at[4 + 2 * rounds])


def finish(both, dist_ref, mean_ref):
    count = dist_ref.shape[0]
    dist_ref[...] = both[pl.ds(0, count), :]
    mean_ref[...] = both[pl.ds(count, 1), : mean_ref.shape[1]]


def body(embeddings, prior_dist, seed_ids):
    rows, width = embeddings.shape
    rounds, seeds = seed_ids.shape
    groups, devs = lax.axis_size("grp"), lax.axis_size("dev")
    share = seeds // devs
    slots = -(-rounds // groups)
    sizes = (groups, devs, rounds, seeds, rows, width)
    flat = (rows // LANES, LANES)
    vmem = pl.BlockSpec(memory_space=pltpu.VMEM)
    hbm = pl.BlockSpec(memory_space=pltpu.HBM)
    inputs = (seed_ids, embeddings, prior_dist.reshape(flat))
    both = pl.pallas_call(
        functools.partial(kernel, sizes),
        name="seeding",
        out_shape=jax.ShapeDtypeStruct((rows // LANES + 8, LANES), jnp.float32),
        in_specs=[hbm, hbm, hbm],
        out_specs=vmem,
        scratch_shapes=[
            pltpu.VMEM((slots, 1, seeds), jnp.int32),
            pltpu.VMEM((slots, 1, seeds), jnp.int32),
            [pltpu.SMEM((1, seeds), jnp.int32)] * slots,
            pltpu.VMEM((rows, width), jnp.bfloat16),
            pltpu.VMEM(flat, jnp.float32),
            pltpu.VMEM((2 * rows + 2 * EDGE, LANES), jnp.float32),
            pltpu.VMEM((2 * seeds, LANES), jnp.float32),
            pltpu.VMEM((slots, 2, devs // 2, share, width), jnp.bfloat16),
            pltpu.VMEM((slots, devs // 2, share, width), jnp.bfloat16),
            pltpu.VMEM((slots, devs // 2, share, width), jnp.bfloat16),
            pltpu.VMEM((slots, devs // 2, share, width), jnp.bfloat16),
            pltpu.VMEM((rounds, share, width), jnp.bfloat16),
            pltpu.VMEM((rounds, 2, devs // 2, share, width), jnp.bfloat16),
            pltpu.VMEM((2 * UNROLL, seeds // 2, LANES), jnp.float32),
            pltpu.VMEM(flat, jnp.float32),
            pltpu.VMEM((rounds, *flat), jnp.float32),
            pltpu.VMEM((8, LANES), jnp.float32),
            pltpu.VMEM((1, LANES), jnp.float32),
            pltpu.VMEM((devs, 1, LANES), jnp.float32),
            pltpu.SemaphoreType.DMA((8,)),
            pltpu.SemaphoreType.DMA((slots,)),
            pltpu.SemaphoreType.DMA((slots,)),
            pltpu.SemaphoreType.DMA,
            pltpu.SemaphoreType.DMA((7 + 2 * rounds,)),
            pltpu.SemaphoreType.DMA((2,)),
            pltpu.SemaphoreType.DMA((2,)),
            pltpu.SemaphoreType.DMA((rounds,)),
            pltpu.SemaphoreType.DMA((rounds,)),
            pltpu.SemaphoreType.DMA((rounds,)),
            pltpu.SemaphoreType.DMA,
        ],
        compiler_params=pltpu.CompilerParams(
            collective_id=0, has_side_effects=True, vmem_limit_bytes=48 * 1024 * 1024
        ),
    )(*(pltpu.with_memory_space_constraint(x, pltpu.HBM) for x in inputs))
    dist, means = pl.pallas_call(
        finish,
        name="finish",
        out_shape=(
            jax.ShapeDtypeStruct(flat, jnp.float32),
            jax.ShapeDtypeStruct((1, rounds), jnp.float32),
        ),
        in_specs=[vmem],
        out_specs=(vmem, vmem),
        compiler_params=pltpu.CompilerParams(vmem_limit_bytes=1024 * 1024),
    )(both)
    return dist.reshape(rows), means.reshape(rounds, 1)


def solution(mesh):
    placed = (P(("grp", "dev"), None), P(("grp", "dev")), P())
    return jax.shard_map(
        body,
        mesh=mesh,
        in_specs=placed,
        out_specs=(P(("grp", "dev")), P(None, "grp")),
        check_vma=False,
    )
```
